8 devices in a mesh: dp: 2 (over z, y), tp: 4 (over x, core).
Axes of the slice: x: 2, y: 2, z: 1, core: 2. Of those that a mesh axis runs over, the one named last changes fastest.
Arguments:
- x_in: bfloat16 [8, 1024, 1280], P('dp', 'tp'), parts along dimension 0
- grad_y: bfloat16 [8, 1024, 1280], P('dp', 'tp'), parts along dimension 0
- pad_mask: int32 [8, 1024], P('dp'), parts along dimension 0
- ln1_gain: float32 [1280], replicated
- ln1_bias: float32 [1280], replicated
- w_qkv: bfloat16 [3, 1280, 20, 64], P(None, None, 'tp')
- b_qkv: float32 [3, 20, 64], P(None, 'tp')
- w_out: bfloat16 [20, 64, 1280], P('tp')
- b_out: float32 [1280], replicated
- ln2_gain: float32 [1280], replicated
- ln2_bias: float32 [1280], replicated
- w_up: bfloat16 [1280, 5120], P(None, 'tp')
- b_up: float32 [5120], P('tp')
- w_down: bfloat16 [5120, 1280], P('tp')
- b_down: float32 [1280], replicated
Outputs:
- output 1: bfloat16 [8, 1024, 1280], P('dp', 'tp'), parts along dimension 0
- output 2: bfloat16 [8, 1024, 1280], P('dp', 'tp'), parts along dimension 0
- output 3: float32 [2560], P('dp'), parts along dimension 0
- output 4: float32 [2560], P('dp'), parts along dimension 0
- output 5: float32 [6, 1280, 20, 64], P('dp', None, 'tp'), parts along dimension 0
- output 6: float32 [6, 20, 64], P('dp', 'tp'), parts along dimension 0
- output 7: float32 [40, 64, 1280], P(('dp', 'tp')), parts along dimension 0
- output 8: float32 [2560], P('dp'), parts along dimension 0
- output 9: float32 [2560], P('dp'), parts along dimension 0
- output 10: float32 [2560], P('dp'), parts along dimension 0
- output 11: float32 [2560, 5120], P('dp', 'tp'), parts along dimension 0
- output 12: float32 [10240], P(('dp', 'tp')), parts along dimension 0
- output 13: float32 [10240, 1280], P(('dp', 'tp')), parts along dimension 0
- output 14: float32 [2560], P('dp'), parts along dimension 0
There are 2 independent parts. The reference program is written for one: setup_inputs(seed, part) draws one part's arguments, and reference() takes and returns one part's arrays. A program takes and returns all parts, laid end to end along the dimension named above; an argument that names none is the same for every part.
All inputs are finite; a program needn't handle non-finite values.
Results may differ from the reference program's by a relative error of at most 0.0124897.
Values are sent between devices in bfloat16 or wider.
A program may use at most 1 GiB of HBM per device.

```python
import jax
import jax.numpy as jnp
from jax import lax

BATCH_SEQS = 4
SEQ_LEN = 1024
MODEL_DIM = 1280
NUM_HEADS = 20
HEAD_DIM = 64
FFN_DIM = 5120
HALF_DIM = HEAD_DIM // 2
TOKENS = BATCH_SEQS * SEQ_LEN
LN_EPS = 1e-5
ROPE_BASE = 10000.0
INV_SQRT2 = 0.7071067811865476
INV_SQRT_2PI = 0.3989422804014327
NEG_LARGE = -1e30


def setup_inputs(seed: int = 0, part: int = 0) -> dict:
    root_key = jax.random.key(seed)
    shared_key, data_key = jax.random.split(root_key)
    weight_keys = jax.random.split(shared_key, 12)
    part_key = jax.random.fold_in(data_key, part)
    data_keys = jax.random.split(part_key, 4)
    tok_shape = (BATCH_SEQS, SEQ_LEN, MODEL_DIM)
    row_scale = 0.5 + jax.random.uniform(data_keys[0], (BATCH_SEQS, SEQ_LEN, 1), jnp.float32)
    x_in = (jax.random.normal(data_keys[1], tok_shape, jnp.float32) * row_scale).astype(jnp.bfloat16)
    grad_y = jax.random.normal(data_keys[2], tok_shape, jnp.float32).astype(jnp.bfloat16)
    lengths = jax.random.randint(data_keys[3], (BATCH_SEQS,), SEQ_LEN // 8, SEQ_LEN + 1)
    pad_mask = (jnp.arange(SEQ_LEN)[None, :] < lengths[:, None]).astype(jnp.int32)
    qkv_gain = jnp.array([1.5, 1.5, 1.0], jnp.float32)[:, None, None, None]
    w_qkv = jax.random.normal(weight_keys[0], (3, MODEL_DIM, NUM_HEADS, HEAD_DIM), jnp.float32) * qkv_gain * MODEL_DIM ** -0.5
    w_out = jax.random.normal(weight_keys[1], (NUM_HEADS, HEAD_DIM, MODEL_DIM), jnp.float32) * MODEL_DIM ** -0.5
    w_up = jax.random.normal(weight_keys[2], (MODEL_DIM, FFN_DIM), jnp.float32) * MODEL_DIM ** -0.5
    w_down = jax.random.normal(weight_keys[3], (FFN_DIM, MODEL_DIM), jnp.float32) * FFN_DIM ** -0.5
    return {
        'x_in': x_in,
        'grad_y': grad_y,
        'pad_mask': pad_mask,
        'ln1_gain': 1.0 + 0.2 * jax.random.normal(weight_keys[4], (MODEL_DIM,), jnp.float32),
        'ln1_bias': 0.2 * jax.random.normal(weight_keys[5], (MODEL_DIM,), jnp.float32),
        'w_qkv': w_qkv.astype(jnp.bfloat16),
        'b_qkv': 0.5 * jax.random.normal(weight_keys[6], (3, NUM_HEADS, HEAD_DIM), jnp.float32),
        'w_out': w_out.astype(jnp.bfloat16),
        'b_out': 0.3 * jax.random.normal(weight_keys[7], (MODEL_DIM,), jnp.float32),
        'ln2_gain': 1.0 + 0.2 * jax.random.normal(weight_keys[8], (MODEL_DIM,), jnp.float32),
        'ln2_bias': 0.2 * jax.random.normal(weight_keys[9], (MODEL_DIM,), jnp.float32),
        'w_up': w_up.astype(jnp.bfloat16),
        'b_up': 0.5 * jax.random.normal(weight_keys[10], (FFN_DIM,), jnp.float32),
        'w_down': w_down.astype(jnp.bfloat16),
        'b_down': 0.3 * jax.random.normal(weight_keys[11], (MODEL_DIM,), jnp.float32),
    }


def layer_norm(values, ln_gain, ln_bias):
    centered = values - jnp.mean(values, axis=-1, keepdims=True)
    inv_std = lax.rsqrt(jnp.mean(centered * centered, axis=-1, keepdims=True) + LN_EPS)
    x_hat = centered * inv_std
    return x_hat * ln_gain + ln_bias, x_hat, inv_std


def layer_norm_grad(d_out, x_hat, inv_std, ln_gain):
    d_hat = d_out * ln_gain
    return inv_std * (d_hat - jnp.mean(d_hat, axis=-1, keepdims=True) - x_hat * jnp.mean(d_hat * x_hat, axis=-1, keepdims=True))


def rope_tables():
    inv_freq = ROPE_BASE ** (-2.0 * jnp.arange(HALF_DIM, dtype=jnp.float32) / HEAD_DIM)
    angles = jnp.arange(SEQ_LEN, dtype=jnp.float32)[:, None] * inv_freq[None, :]
    angles = jnp.concatenate([angles, angles], axis=-1)
    return jnp.cos(angles)[:, None, :], jnp.sin(angles)[:, None, :]


def rotate(tensor, cos_tab, sin_tab):
    swapped = jnp.concatenate([-tensor[..., HALF_DIM:], tensor[..., :HALF_DIM]], axis=-1)
    return tensor * cos_tab + swapped * sin_tab


def rotate_back(grad_in, cos_tab, sin_tab):
    scaled = grad_in * sin_tab
    swapped = jnp.concatenate([scaled[..., HALF_DIM:], -scaled[..., :HALF_DIM]], axis=-1)
    return grad_in * cos_tab + swapped


def attention_probs(q_seq, k_seq, key_ok):
    scores = jnp.einsum('qhk,shk->hqs', q_seq.astype(jnp.float32), k_seq.astype(jnp.float32))
    return jax.nn.softmax(jnp.where(key_ok[None, None, :], scores, NEG_LARGE), axis=-1)


def seq_attention(operands):
    q_seq, k_seq, v_seq, key_ok = operands
    probs_low = attention_probs(q_seq, k_seq, key_ok).astype(jnp.bfloat16)
    return jnp.einsum('hqs,shk->qhk', probs_low.astype(jnp.float32), v_seq.astype(jnp.float32)).astype(jnp.bfloat16)


def seq_attention_grad(operands):
    q_seq, k_seq, v_seq, key_ok, d_out = operands
    attn_probs = attention_probs(q_seq, k_seq, key_ok)
    probs_low = attn_probs.astype(jnp.bfloat16).astype(jnp.float32)
    d_out_f = d_out.astype(jnp.float32)
    d_value = jnp.einsum('hqs,qhk->shk', probs_low, d_out_f)
    d_probs = jnp.einsum('qhk,shk->hqs', d_out_f, v_seq.astype(jnp.float32))
    d_scores = attn_probs * (d_probs - jnp.sum(d_probs * attn_probs, axis=-1, keepdims=True))
    d_scores_low = d_scores.astype(jnp.bfloat16).astype(jnp.float32)
    d_query = jnp.einsum('hqs,shk->qhk', d_scores_low, k_seq.astype(jnp.float32))
    d_key = jnp.einsum('hqs,qhk->shk', d_scores_low, q_seq.astype(jnp.float32))
    return d_query, d_key, d_value


def reference(x_in, grad_y, pad_mask, ln1_gain, ln1_bias, w_qkv, b_qkv, w_out, b_out, ln2_gain, ln2_bias, w_up, b_up, w_down, b_down):
    q_scale = HEAD_DIM ** -0.5
    cos_tab, sin_tab = rope_tables()
    key_ok = pad_mask > 0
    x_f = x_in.astype(jnp.float32)
    h1_f, x_hat1, inv_std1 = layer_norm(x_f, ln1_gain, ln1_bias)
    h1_b = h1_f.astype(jnp.bfloat16)
    qkv_all = jnp.einsum('bsd,idhk->ibshk', h1_b.astype(jnp.float32), w_qkv.astype(jnp.float32)) + b_qkv[:, None, None]
    q_rot = rotate(qkv_all[0] * q_scale, cos_tab, sin_tab).astype(jnp.bfloat16)
    k_rot = rotate(qkv_all[1], cos_tab, sin_tab).astype(jnp.bfloat16)
    v_heads = qkv_all[2].astype(jnp.bfloat16)
    attn_o = lax.map(seq_attention, (q_rot, k_rot, v_heads, key_ok))
    attn_sum = jnp.einsum('bshk,hkd->bsd', attn_o.astype(jnp.float32), w_out.astype(jnp.float32)) + b_out
    x1_f = (x_f + attn_sum).astype(jnp.bfloat16).astype(jnp.float32)
    h2_f, x_hat2, inv_std2 = layer_norm(x1_f, ln2_gain, ln2_bias)
    h2_flat = h2_f.astype(jnp.bfloat16).reshape(TOKENS, MODEL_DIM)
    pre_act = jnp.dot(h2_flat, w_up, preferred_element_type=jnp.float32) + b_up
    erf_term = lax.erf(pre_act * INV_SQRT2)
    act_b = (0.5 * pre_act * (1.0 + erf_term)).astype(jnp.bfloat16)
    gelu_slope = 0.5 * (1.0 + erf_term) + pre_act * jnp.exp(-0.5 * pre_act * pre_act) * INV_SQRT_2PI
    mlp_sum = jnp.dot(act_b, w_down, preferred_element_type=jnp.float32) + b_down
    y_out = (x1_f + mlp_sum.reshape(x_f.shape)).astype(jnp.bfloat16)
    dy_flat = grad_y.reshape(TOKENS, MODEL_DIM)
    dy_f = grad_y.astype(jnp.float32)
    grad_b_down = jnp.sum(dy_f, axis=(0, 1))
    grad_w_down = jnp.dot(act_b.T, dy_flat, preferred_element_type=jnp.float32)
    d_act = jnp.dot(dy_flat, w_down.T, preferred_element_type=jnp.float32)
    d_pre = d_act * gelu_slope
    grad_b_up = jnp.sum(d_pre, axis=0)
    d_pre_b = d_pre.astype(jnp.bfloat16)
    grad_w_up = jnp.dot(h2_flat.T, d_pre_b, preferred_element_type=jnp.float32)
    d_h2 = jnp.dot(d_pre_b, w_up.T, preferred_element_type=jnp.float32).reshape(x_f.shape)
    grad_ln2_gain = jnp.sum(d_h2 * x_hat2, axis=(0, 1))
    grad_ln2_bias = jnp.sum(d_h2, axis=(0, 1))
    d_x1 = dy_f + layer_norm_grad(d_h2, x_hat2, inv_std2, ln2_gain)
    grad_b_out = jnp.sum(d_x1, axis=(0, 1))
    d_x1_b = d_x1.astype(jnp.bfloat16).astype(jnp.float32)
    grad_w_out = jnp.einsum('bshk,bsd->hkd', attn_o.astype(jnp.float32), d_x1_b)
    d_attn_o = jnp.einsum('bsd,hkd->bshk', d_x1_b, w_out.astype(jnp.float32)).astype(jnp.bfloat16)
    d_query, d_key, d_value = lax.map(seq_attention_grad, (q_rot, k_rot, v_heads, key_ok, d_attn_o))
    d_qkv = jnp.stack([rotate_back(d_query, cos_tab, sin_tab) * q_scale, rotate_back(d_key, cos_tab, sin_tab), d_value])
    grad_b_qkv = jnp.sum(d_qkv, axis=(1, 2))
    d_qkv_b = d_qkv.astype(jnp.bfloat16).astype(jnp.float32)
    grad_w_qkv = jnp.einsum('bsd,ibshk->idhk', h1_b.astype(jnp.float32), d_qkv_b)
    d_h1 = jnp.einsum('ibshk,idhk->bsd', d_qkv_b, w_qkv.astype(jnp.float32))
    grad_ln1_gain = jnp.sum(d_h1 * x_hat1, axis=(0, 1))
    grad_ln1_bias = jnp.sum(d_h1, axis=(0, 1))
    grad_x = (d_x1 + layer_norm_grad(d_h1, x_hat1, inv_std1, ln1_gain)).astype(jnp.bfloat16)
    return (y_out, grad_x, grad_ln1_gain, grad_ln1_bias, grad_w_qkv, grad_b_qkv, grad_w_out, grad_b_out, grad_ln2_gain, grad_ln2_bias, grad_w_up, grad_b_up, grad_w_down, grad_b_down)
```

```python
import functools

import jax
import jax.numpy as jnp
from jax import lax
from jax.experimental import pallas as pl
from jax.experimental.pallas import tpu as pltpu
from jax.sharding import PartitionSpec as P

LN_EPS = 1e-5
ROPE_BASE = 10000.0
INV_SQRT2 = 0.7071067811865476
INV_SQRT_2PI = 0.3989422804014327
NEG_LARGE = -1e30
F32 = jnp.float32
BF16 = jnp.bfloat16
NT = (((1,), (1,)), ((), ()))
VMEM_LIMIT = 60 * 1024 * 1024
QB = 256


def layer_norm(values, ln_gain, ln_bias):
    centered = values - jnp.mean(values, axis=-1, keepdims=True)
    inv_std = lax.rsqrt(jnp.mean(centered * centered, axis=-1, keepdims=True) + LN_EPS)
    x_hat = centered * inv_std
    return x_hat * ln_gain + ln_bias, x_hat, inv_std


def layer_norm_grad(d_out, x_hat, inv_std, ln_gain):
    d_hat = d_out * ln_gain
    return inv_std * (d_hat - jnp.mean(d_hat, axis=-1, keepdims=True) - x_hat * jnp.mean(d_hat * x_hat, axis=-1, keepdims=True))


def rope_tables(seq_len, head_dim):
    half_dim = head_dim // 2
    inv_freq = ROPE_BASE ** (-2.0 * jnp.arange(half_dim, dtype=F32) / head_dim)
    angles = jnp.arange(seq_len, dtype=F32)[:, None] * inv_freq[None, :]
    cos_half, sin_half = jnp.cos(angles), jnp.sin(angles)
    cos_tab = jnp.concatenate([cos_half] * 4, axis=-1)
    sin_tab = jnp.concatenate([-sin_half, sin_half, -sin_half, sin_half], axis=-1)
    return cos_tab, sin_tab


def swap_halves(t, first_half):
    return jnp.where(first_half, pltpu.roll(t, 96, 1), pltpu.roll(t, 32, 1))


def pair_rows(ref0, ref1):
    return jnp.concatenate([r[i] for i in range(3) for r in (ref0, ref1)], axis=0)


def attn_fwd_kernel(h_ref, w0_ref, w1_ref, b_ref, cos_ref, sin_ref, mb_ref, wo0_ref, wo1_ref,
                    q_ref, k_ref, v_ref, o_ref, lse_ref, acc_ref, qs, ks, st):
    seq = h_ref.shape[0]
    lane = lax.broadcasted_iota(jnp.int32, (1, 128), 1)
    first_half = (lane % 64) < 32
    head0 = lane < 64
    w = pair_rows(w0_ref, w1_ref)
    t = lax.dot_general(h_ref[...], w, NT, preferred_element_type=F32)
    cos, sin = cos_ref[...], sin_ref[...]
    tq = (t[:, :128] + b_ref[0, 0:1]) * 0.125
    tk = t[:, 128:256] + b_ref[0, 1:2]
    q = (tq * cos + swap_halves(tq, first_half) * sin).astype(BF16)
    k = (tk * cos + swap_halves(tk, first_half) * sin).astype(BF16)
    v_ref[...] = (t[:, 256:] + b_ref[0, 2:3]).astype(BF16)
    q_ref[...] = q
    k_ref[...] = k
    q, k = q.astype(F32), k.astype(F32)
    mb = mb_ref[...]
    qs[0] = jnp.where(head0, q, jnp.where(lane == 64, 1.0, 0.0)).astype(BF16)
    qs[1] = jnp.where(head0, jnp.where(lane == 0, 1.0, 0.0), q).astype(BF16)
    ks[0] = jnp.where(head0, k, jnp.where(lane == 64, mb, 0.0)).astype(BF16)
    ks[1] = jnp.where(head0, jnp.where(lane == 0, mb, 0.0), k).astype(BF16)

    def block(j, carry):
        rows = pl.ds(pl.multiple_of(j * QB, QB), QB)
        outs, stats = [], []
        for head in range(2):
            s = lax.dot_general(qs[head, rows, :], ks[head], NT, preferred_element_type=F32)
            m = jnp.max(s, axis=-1, keepdims=True)
            e = jnp.exp(s - m)
            total = jnp.sum(e, axis=-1, keepdims=True)
            p = (e * (1.0 / total)).astype(BF16)
            outs.append(jnp.dot(p, v_ref[...], preferred_element_type=F32))
            stats.append(m + jnp.log(total))
        o_ref[rows, :] = jnp.where(head0, outs[0], outs[1]).astype(BF16)
        st[rows, :] = jnp.where(head0, stats[0], stats[1])
        return carry

    lax.fori_loop(0, seq // QB, block, 0)
    st_t = st[...].T
    lse_ref[0] = jnp.concatenate([st_t[0:1]] * 4 + [st_t[64:65]] * 4, axis=0)
    wo = jnp.concatenate([wo0_ref[0], wo1_ref[0]], axis=0)
    part = jnp.dot(o_ref[...], wo, preferred_element_type=F32)

    @pl.when(pl.program_id(0) == 0)
    def _():
        acc_ref[...] = part

    @pl.when(pl.program_id(0) > 0)
    def _():
        acc_ref[...] += part


def attn_fwd(h1, w0, w1, bias, cos_tab, sin_tab, mask_col, wo0, wo1):
    seq, dim = h1.shape
    heads = w0.shape[1] // 64
    full = lambda i: (0, 0)
    pair = pl.BlockSpec((seq, 128), lambda i: (0, i))
    head_w = pl.BlockSpec((3, 64, dim), lambda i: (0, i, 0))
    head_o = pl.BlockSpec((1, 64, dim), lambda i: (i, 0, 0))
    act = jax.ShapeDtypeStruct((seq, heads * 128), BF16)
    return pl.pallas_call(
        attn_fwd_kernel,
        grid=(heads,),
        in_specs=[pl.BlockSpec((seq, dim), full), head_w, head_w, pl.BlockSpec((1, 3, 128), lambda i: (i, 0, 0)),
                  pl.BlockSpec((seq, 128), full), pl.BlockSpec((seq, 128), full), pl.BlockSpec((seq, 128), full), head_o, head_o],
        out_specs=[pair, pair, pair, pair, pl.BlockSpec((1, 8, seq), lambda i: (i, 0, 0)), pl.BlockSpec((seq, dim), full)],
        out_shape=[act, act, act, act, jax.ShapeDtypeStruct((heads, 8, seq), F32), jax.ShapeDtypeStruct((seq, dim), F32)],
        scratch_shapes=[pltpu.VMEM((2, seq, 128), BF16), pltpu.VMEM((2, seq, 128), BF16), pltpu.VMEM((seq, 128), F32)],
        compiler_params=pltpu.CompilerParams(dimension_semantics=("arbitrary",), vmem_limit_bytes=VMEM_LIMIT),
        cost_estimate=pl.CostEstimate(flops=heads * 2 * seq * (dim * 512 + 4 * seq * 256), bytes_accessed=20_000_000, transcendentals=0),
        name="attn_fwd",
    )(h1, w0, w1, bias, cos_tab, sin_tab, mask_col, wo0, wo1)


def attn_bwd_kernel(h_ref, dx_ref, w0_ref, w1_ref, wo0_ref, wo1_ref, q_ref, k_ref, v_ref, o_ref, lse_ref, cos_ref, sin_ref, mb_ref,
                    dh_ref, gw0_ref, gw1_ref, gwo0_ref, gwo1_ref, gb_ref, qs, qz, ks, dos, kt, dqt, dk_acc, dv_acc):
    seq, dim = h_ref.shape
    lane = lax.broadcasted_iota(jnp.int32, (1, 128), 1)
    first_half = (lane % 64) < 32
    head0 = lane < 64
    dx = dx_ref[...]
    wo = jnp.concatenate([wo0_ref[0], wo1_ref[0]], axis=0)
    d_o = lax.dot_general(dx, wo, NT, preferred_element_type=F32)
    dos[0] = jnp.where(head0, d_o, 0.0).astype(BF16)
    dos[1] = jnp.where(head0, 0.0, d_o).astype(BF16)
    gwo = jnp.dot(o_ref[...].T, dx, preferred_element_type=F32)
    gwo0_ref[0] = gwo[:64]
    gwo1_ref[0] = gwo[64:]
    q, k, mb = q_ref[...].astype(F32), k_ref[...].astype(F32), mb_ref[...]
    qs[0] = jnp.where(head0, q, jnp.where(lane == 64, 1.0, 0.0)).astype(BF16)
    qs[1] = jnp.where(head0, jnp.where(lane == 0, 1.0, 0.0), q).astype(BF16)
    qz[0] = jnp.where(head0, q, 0.0).astype(BF16)
    qz[1] = jnp.where(head0, 0.0, q).astype(BF16)
    ks[0] = jnp.where(head0, k, jnp.where(lane == 64, mb, 0.0)).astype(BF16)
    ks[1] = jnp.where(head0, jnp.where(lane == 0, mb, 0.0), k).astype(BF16)
    kt[...] = k_ref[...].T
    dk_acc[...] = jnp.zeros_like(dk_acc)
    dv_acc[...] = jnp.zeros_like(dv_acc)

    def block(j, carry):
        rows = pl.ds(pl.multiple_of(j * QB, QB), QB)
        for head in range(2):
            s_t = lax.dot_general(ks[head], qs[head, rows, :], NT, preferred_element_type=F32)
            p_t = jnp.exp(s_t - lse_ref[0, 4 * head:4 * head + 1, rows])
            do_b = dos[head, rows, :]
            dp_t = lax.dot_general(v_ref[...], do_b, NT, preferred_element_type=F32)
            corr = jnp.sum(p_t * dp_t, axis=0, keepdims=True)
            ds_t = (p_t * (dp_t - corr)).astype(BF16)
            dv_acc[...] += jnp.dot(p_t.astype(BF16), do_b, preferred_element_type=F32)
            dk_acc[...] += jnp.dot(ds_t, qz[head, rows, :], preferred_element_type=F32)
            dqt[64 * head:64 * head + 64, rows] = jnp.dot(kt[64 * head:64 * head + 64, :], ds_t, preferred_element_type=F32)
        return carry

    lax.fori_loop(0, seq // QB, block, 0)
    cos, sin = cos_ref[...], sin_ref[...]
    dq, dk, dv = dqt[...].T, dk_acc[...], dv_acc[...]
    dq = (dq * cos - swap_halves(dq, first_half) * sin) * 0.125
    dk = dk * cos - swap_halves(dk, first_half) * sin
    d_all = jnp.concatenate([dq, dk, dv], axis=1)
    sums = jnp.sum(d_all, axis=0, keepdims=True)
    gb_ref[0] = jnp.concatenate([sums[:, :128], sums[:, 128:256], sums[:, 256:], jnp.zeros((5, 128), F32)], axis=0)
    d_low = d_all.astype(BF16)
    w = pair_rows(w0_ref, w1_ref)
    part = jnp.dot(d_low, w, preferred_element_type=F32)
    gw = jnp.dot(d_low.T, h_ref[...], preferred_element_type=F32)
    for i in range(3):
        gw0_ref[i] = gw[128 * i:128 * i + 64]
        gw1_ref[i] = gw[128 * i + 64:128 * i + 128]

    @pl.when(pl.program_id(0) == 0)
    def _():
        dh_ref[...] = part

    @pl.when(pl.program_id(0) > 0)
    def _():
        dh_ref[...] += part


def attn_bwd(h1, d_x1, w0, w1, wo0, wo1, q, k, v, o, lse, cos_tab, sin_tab, mask_col):
    seq, dim = h1.shape
    heads = w0.shape[1] // 64
    full = lambda i: (0, 0)
    pair = pl.BlockSpec((seq, 128), lambda i: (0, i))
    head_w = pl.BlockSpec((3, 64, dim), lambda i: (0, i, 0))
    head_o = pl.BlockSpec((1, 64, dim), lambda i: (i, 0, 0))
    tab = pl.BlockSpec((seq, 128), full)
    gw = jax.ShapeDtypeStruct((3, heads * 64, dim), F32)
    gwo = jax.ShapeDtypeStruct((heads, 64, dim), F32)
    half = pltpu.VMEM((2, seq, 128), BF16)
    return pl.pallas_call(
        attn_bwd_kernel,
        grid=(heads,),
        in_specs=[pl.BlockSpec((seq, dim), full), pl.BlockSpec((seq, dim), full), head_w, head_w, head_o, head_o, pair, pair, pair, pair,
                  pl.BlockSpec((1, 8, seq), lambda i: (i, 0, 0)), tab, tab, tab],
        out_specs=[pl.BlockSpec((seq, dim), full), head_w, head_w, head_o, head_o, pl.BlockSpec((1, 8, 128), lambda i: (i, 0, 0))],
        out_shape=[jax.ShapeDtypeStruct((seq, dim), F32), gw, gw, gwo, gwo, jax.ShapeDtypeStruct((heads, 8, 128), F32)],
        scratch_shapes=[half, half, half, half, pltpu.VMEM((128, seq), BF16), pltpu.VMEM((128, seq), F32),
                        pltpu.VMEM((seq, 128), F32), pltpu.VMEM((seq, 128), F32)],
        compiler_params=pltpu.CompilerParams(dimension_semantics=("arbitrary",), vmem_limit_bytes=VMEM_LIMIT),
        cost_estimate=pl.CostEstimate(flops=heads * 2 * seq * (dim * 1024 + 10 * seq * 256), bytes_accessed=40_000_000, transcendentals=0),
        name="attn_bwd",
    )(h1, d_x1, w0, w1, wo0, wo1, q, k, v, o, lse, cos_tab, sin_tab, mask_col)


def gelu_terms(pre):
    erf_term = lax.erf(pre * INV_SQRT2)
    act = 0.5 * pre * (1.0 + erf_term)
    slope = 0.5 * (1.0 + erf_term) + pre * jnp.exp(-0.5 * pre * pre) * INV_SQRT_2PI
    return act, slope


def mlp_kernel(tiles, n_w, *refs):
    h_ref, dy_ref, b_ref = refs[:3]
    up_refs, down_refs = refs[3:3 + n_w], refs[3 + n_w:3 + 2 * n_w]
    y_ref, dh_ref, wu, wd, sem = refs[3 + 2 * n_w:]
    seq = h_ref.shape[0]
    width = wu.shape[2]
    copies = []
    for t, (src, part) in enumerate(tiles):
        cols = pl.ds(part * width, width)
        copies.append((pltpu.make_async_copy(up_refs[src].at[:, cols], wu.at[t], sem.at[0, t]),
                       pltpu.make_async_copy(down_refs[src].at[cols, :], wd.at[t], sem.at[1, t])))
    for pair in copies:
        pair[0].start()
        pair[1].start()
    for t in range(len(tiles)):
        copies[t][0].wait()
        copies[t][1].wait()

        def block(j, carry, t=t):
            rows = pl.ds(pl.multiple_of(j * QB, QB), QB)
            pre = jnp.dot(h_ref[rows, :], wu[t], preferred_element_type=F32) + b_ref[t]
            act, slope = gelu_terms(pre)
            d_act = lax.dot_general(dy_ref[rows, :], wd[t], NT, preferred_element_type=F32)
            y_part = jnp.dot(act.astype(BF16), wd[t], preferred_element_type=F32)
            d_pre = (d_act * slope).astype(BF16)
            dh_part = lax.dot_general(d_pre, wu[t], NT, preferred_element_type=F32)
            if t == 0:
                y_ref[rows, :] = y_part
                dh_ref[rows, :] = dh_part
            else:
                y_ref[rows, :] += y_part
                dh_ref[rows, :] += dh_part
            return carry

        lax.fori_loop(0, seq // QB, block, 0)


def mlp_chain(h2, d_y, bias, ups, downs):
    seq, dim = h2.shape
    width = 640
    tiles = [(i, p) for i, w in enumerate(ups) for p in range(w.shape[1] // width)]
    vmem, hbm = pl.BlockSpec(memory_space=pltpu.VMEM), pl.BlockSpec(memory_space=pl.ANY)
    out = jax.ShapeDtypeStruct((seq, dim), F32)
    return pl.pallas_call(
        functools.partial(mlp_kernel, tiles, len(ups)),
        in_specs=[vmem, vmem, vmem] + [hbm] * (2 * len(ups)),
        out_specs=[vmem, vmem],
        out_shape=[out, out],
        scratch_shapes=[pltpu.VMEM((len(tiles), dim, width), BF16), pltpu.VMEM((len(tiles), width, dim), BF16),
                        pltpu.SemaphoreType.DMA((2, len(tiles)))],
        compiler_params=pltpu.CompilerParams(vmem_limit_bytes=VMEM_LIMIT),
        cost_estimate=pl.CostEstimate(flops=len(tiles) * 8 * seq * dim * width, bytes_accessed=30_000_000, transcendentals=0),
        name="mlp_chain",
    )(h2, d_y, bias.reshape(len(tiles), 1, width), *ups, *downs)


def xor_move(value, bits):
    return lax.ppermute(value, 'tp', [(i, i ^ bits) for i in range(4)])


def swap_groups(value):
    return lax.ppermute(value, 'dp', [(0, 1), (1, 0)])


def cross_halves(shard, axis, group):
    size = shard.shape[axis] // 2
    piece = xor_move(lax.dynamic_slice_in_dim(shard, group * size, size, axis), 2)
    return piece, swap_groups(piece)


def cross_ordered(shard, axis, group):
    here, there = cross_halves(shard, axis, group)
    return jnp.concatenate([jnp.where(group == 0, here, there), jnp.where(group == 0, there, here)], axis=axis)


def solution(mesh):
    act_spec = P('dp', 'tp', None)
    rep_vec = P(None)
    part_vec = P('dp')
    in_specs = (act_spec, act_spec, P('dp', None), rep_vec, rep_vec, P(None, None, 'tp', None), P(None, 'tp', None),
                P('tp', None, None), rep_vec, rep_vec, rep_vec, P(None, 'tp'), P('tp'), P('tp', None), rep_vec)
    out_specs = (act_spec, act_spec, part_vec, part_vec, P('dp', None, 'tp', None), P('dp', 'tp', None),
                 P(('dp', 'tp'), None, None), part_vec, part_vec, part_vec, P('dp', 'tp'), P(('dp', 'tp')),
                 P(('dp', 'tp'), None), part_vec)

    def device_step(x_in, grad_y, pad_mask, ln1_gain, ln1_bias, w_qkv, b_qkv, w_out, b_out, ln2_gain, ln2_bias, w_up, b_up, w_down, b_down):
        me = lax.axis_index('tp')
        group = lax.axis_index('dp')
        n_seq, rows, dim = x_in.shape
        seq = pad_mask.shape[1]
        heads = w_out.shape[0]
        cols = w_up.shape[1]
        cos_tab, sin_tab = rope_tables(seq, 64)

        def to_sequence(blocks):
            out = jnp.zeros((seq, dim), blocks.dtype)
            for s in range(4):
                mine = lax.dynamic_index_in_dim(blocks, me ^ s, 0, keepdims=False)
                got = xor_move(mine, s) if s else mine
                out = lax.dynamic_update_slice_in_dim(out, got, (me ^ s) * rows, 0)
            return out

        def to_blocks(value):
            out = jnp.zeros((n_seq, rows, dim), value.dtype)
            for s in range(4):
                mine = lax.dynamic_slice_in_dim(value, (me ^ s) * rows, rows, 0)
                got = xor_move(mine, s) if s else mine
                out = lax.dynamic_update_index_in_dim(out, got, me ^ s, 0)
            return out

        x_seq = to_sequence(x_in)
        wq = [jnp.transpose(w_qkv, (0, 2, 3, 1)).reshape(3, heads * 64, dim)]
        wq.append(xor_move(wq[0], 1))
        wq.append(cross_ordered(wq[0], 1, group))
        wq.append(xor_move(wq[2], 1))
        wo = [w_out]
        wo.append(xor_move(w_out, 1))
        wo.append(cross_ordered(w_out.reshape(heads * 64, dim), 0, group).reshape(heads, 64, dim))
        wo.append(xor_move(wo[2], 1))
        small = jnp.concatenate([b_up, b_qkv.reshape(-1)])
        smalls = [small] + [xor_move(small, s) for s in (1, 2, 3)]
        b_ups = [v[:cols] for v in smalls]
        b_qkvs = [v[cols:].reshape(3, heads, 64) for v in smalls]
        ups = [w_up, xor_move(w_up, 1)]
        downs = [w_down, xor_move(w_down, 1)]
        dy_full = lax.all_gather(grad_y, 'tp', axis=1, tiled=True)
        up_x = cross_halves(w_up, 1, group)
        down_x = cross_halves(w_down, 0, group)
        ups_x = list(up_x) + [xor_move(v, 1) for v in up_x]
        downs_x = list(down_x) + [xor_move(v, 1) for v in down_x]

        def ordered_bias(v):
            return jnp.where(group == 0, v, jnp.concatenate([v[cols // 2:], v[:cols // 2]]))

        my_mask = lax.dynamic_index_in_dim(pad_mask, me, 0, keepdims=False)
        mask_col = jnp.broadcast_to(jnp.where(my_mask > 0, 0.0, NEG_LARGE).astype(F32)[:, None], (seq, 128))
        x_f = x_seq.astype(F32)
        h1_f, x_hat1, inv_std1 = layer_norm(x_f, ln1_gain, ln1_bias)
        h1 = h1_f.astype(BF16)

        def pair_bias(a, b):
            return jnp.transpose(jnp.concatenate([a, b], axis=-1), (1, 0, 2))

        fwd = [attn_fwd(h1, wq[i], wq[i + 1], pair_bias(b_qkvs[i], b_qkvs[i + 1]), cos_tab, sin_tab, mask_col, wo[i], wo[i + 1])
               for i in (0, 2)]
        x1_f = (x_f + ((fwd[0][5] + fwd[1][5]) + b_out)).astype(BF16).astype(F32)
        h2_f, x_hat2, inv_std2 = layer_norm(x1_f, ln2_gain, ln2_bias)
        h2 = h2_f.astype(BF16)

        d_y = lax.dynamic_index_in_dim(dy_full, me, 0, keepdims=False)
        dy_f = d_y.astype(F32)
        y_a, dh2_a = mlp_chain(h2, d_y, jnp.concatenate([b_ups[0], b_ups[1]]), ups, downs)
        y_b, dh2_b = mlp_chain(h2, d_y, jnp.concatenate([ordered_bias(b_ups[2]), ordered_bias(b_ups[3])]), ups_x, downs_x)
        y_seq = (x1_f + ((y_a + y_b) + b_down)).astype(BF16)
        y_out = to_blocks(y_seq)
        d_h2 = dh2_a + dh2_b
        d_x1 = dy_f + layer_norm_grad(d_h2, x_hat2, inv_std2, ln2_gain)
        d_x1_b = d_x1.astype(BF16)

        bwd = {}
        for i in (2, 0):
            q, k, v, o, lse, _ = fwd[i // 2]
            bwd[i] = attn_bwd(h1, d_x1_b, wq[i], wq[i + 1], wo[i], wo[i + 1], q, k, v, o, lse, cos_tab, sin_tab, mask_col)
        far = [(bwd[2][1], bwd[2][2]), (bwd[2][3], bwd[2][4])]
        near = [(bwd[0][1], bwd[0][2]), (bwd[0][3], bwd[0][4])]
        grads = []
        for (far2, far3), (near0, near1) in zip(far, near):
            across = xor_move(far2 + xor_move(far3, 1), 2)
            grads.append((near0 + xor_move(near1, 1)) + across)
        grad_w_qkv = jnp.transpose(grads[0].reshape(3, heads, 64, dim), (0, 3, 1, 2))
        grad_w_out = grads[1]
        d_h1 = bwd[2][0] + bwd[0][0]
        grad_x_seq = (d_x1 + layer_norm_grad(d_h1, x_hat1, inv_std1, ln1_gain)).astype(BF16)
        grad_x = to_blocks(grad_x_seq)
        gb = []
        for i in (0, 2):
            part = jnp.transpose(bwd[i][5][:, :3], (1, 0, 2))
            gb += [part[..., :64], part[..., 64:]]
        grad_b_qkv = (gb[0] + xor_move(gb[1], 1)) + (xor_move(gb[2], 2) + xor_move(gb[3], 3))

        h2_full = lax.all_gather(h2[None], 'tp', axis=0, tiled=True)
        pre_act = jnp.einsum('bsd,df->bsf', h2_full, w_up, preferred_element_type=F32) + b_up
        act, gelu_slope = gelu_terms(pre_act)
        act_b = act.astype(BF16)
        grad_w_down = jnp.einsum('bsf,bsd->fd', act_b, dy_full, preferred_element_type=F32)
        d_act = jnp.einsum('bsd,fd->bsf', dy_full, w_down, preferred_element_type=F32)
        d_pre = d_act * gelu_slope
        grad_b_up = jnp.sum(d_pre, axis=(0, 1))
        grad_w_up = jnp.einsum('bsd,bsf->df', h2_full, d_pre.astype(BF16), preferred_element_type=F32)

        sums = jnp.stack([jnp.sum(dy_f, axis=0), jnp.sum(d_h2 * x_hat2, axis=0), jnp.sum(d_h2, axis=0), jnp.sum(d_x1, axis=0),
                          jnp.sum(d_h1 * x_hat1, axis=0), jnp.sum(d_h1, axis=0)])
        sums = sums + xor_move(sums, 1)
        sums = sums + xor_move(sums, 2)
        return (y_out, grad_x, sums[4], sums[5], grad_w_qkv, grad_b_qkv, grad_w_out, sums[3],
                sums[1], sums[2], grad_w_up, grad_b_up, grad_w_down, sums[0])

    return jax.shard_map(device_step, mesh=mesh, in_specs=in_specs, out_specs=out_specs, check_vma=False)
```

```python
import functools

import jax
import jax.numpy as jnp
from jax import lax
from jax.experimental import pallas as pl
from jax.experimental.pallas import tpu as pltpu
from jax.sharding import PartitionSpec as P


LN_EPS = 1e-5
ROPE_BASE = 10000.0
INV_SQRT2 = 0.7071067811865476
INV_SQRT_2PI = 0.3989422804014327
NEG_LARGE = -1e30
F32 = jnp.float32
BF16 = jnp.bfloat16
NT = (((1,), (1,)), ((), ()))
VMEM_LIMIT = 60 * 1024 * 1024
QB = 256


def layer_norm(values, ln_gain, ln_bias):
    centered = values - jnp.mean(values, axis=-1, keepdims=True)
    inv_std = lax.rsqrt(jnp.mean(centered * centered, axis=-1, keepdims=True) + LN_EPS)
    x_hat = centered * inv_std
    return x_hat * ln_gain + ln_bias, x_hat, inv_std


def layer_norm_grad(d_out, x_hat, inv_std, ln_gain):
    d_hat = d_out * ln_gain
    return inv_std * (d_hat - jnp.mean(d_hat, axis=-1, keepdims=True) - x_hat * jnp.mean(d_hat * x_hat, axis=-1, keepdims=True))


def rope_tables(seq_len, head_dim):
    half_dim = head_dim // 2
    inv_freq = ROPE_BASE ** (-2.0 * jnp.arange(half_dim, dtype=F32) / head_dim)
    angles = jnp.arange(seq_len, dtype=F32)[:, None] * inv_freq[None, :]
    cos_half, sin_half = jnp.cos(angles), jnp.sin(angles)
    cos_tab = jnp.concatenate([cos_half] * 4, axis=-1)
    sin_tab = jnp.concatenate([-sin_half, sin_half, -sin_half, sin_half], axis=-1)
    return cos_tab, sin_tab


def swap_halves(t, first_half):
    return jnp.where(first_half, pltpu.roll(t, 96, 1), pltpu.roll(t, 32, 1))


def pair_rows(ref0, ref1):
    return jnp.concatenate([r[i] for i in range(3) for r in (ref0, ref1)], axis=0)


def attn_fwd_kernel(h_ref, w0_ref, w1_ref, b_ref, cos_ref, sin_ref, mb_ref, wo0_ref, wo1_ref,
                    q_ref, k_ref, v_ref, o_ref, lse_ref, acc_ref, qs, ks, st):
    seq = h_ref.shape[0]
    lane = lax.broadcasted_iota(jnp.int32, (1, 128), 1)
    first_half = (lane % 64) < 32
    head0 = lane < 64
    w = pair_rows(w0_ref, w1_ref)
    t = lax.dot_general(h_ref[...], w, NT, preferred_element_type=F32)
    cos, sin = cos_ref[...], sin_ref[...]
    tq = (t[:, :128] + b_ref[0, 0:1]) * 0.125
    tk = t[:, 128:256] + b_ref[0, 1:2]
    q = (tq * cos + swap_halves(tq, first_half) * sin).astype(BF16)
    k = (tk * cos + swap_halves(tk, first_half) * sin).astype(BF16)
    v_ref[...] = (t[:, 256:] + b_ref[0, 2:3]).astype(BF16)
    q_ref[...] = q
    k_ref[...] = k
    q, k = q.astype(F32), k.astype(F32)
    mb = mb_ref[...]
    qs[0] = jnp.where(head0, q, jnp.where(lane == 64, 1.0, 0.0)).astype(BF16)
    qs[1] = jnp.where(head0, jnp.where(lane == 0, 1.0, 0.0), q).astype(BF16)
    ks[0] = jnp.where(head0, k, jnp.where(lane == 64, mb, 0.0)).astype(BF16)
    ks[1] = jnp.where(head0, jnp.where(lane == 0, mb, 0.0), k).astype(BF16)

    def block(j, carry):
        rows = pl.ds(pl.multiple_of(j * QB, QB), QB)
        outs, stats = [], []
        for head in range(2):
            s = lax.dot_general(qs[head, rows, :], ks[head], NT, preferred_element_type=F32)
            m = jnp.max(s, axis=-1, keepdims=True)
            e = jnp.exp(s - m)
            total = jnp.sum(e, axis=-1, keepdims=True)
            p = (e * (1.0 / total)).astype(BF16)
            outs.append(jnp.dot(p, v_ref[...], preferred_element_type=F32))
            stats.append(m + jnp.log(total))
        o_ref[rows, :] = jnp.where(head0, outs[0], outs[1]).astype(BF16)
        st[rows, :] = jnp.where(head0, stats[0], stats[1])
        return carry

    lax.fori_loop(0, seq // QB, block, 0)
    st_t = st[...].T
    lse_ref[0] = jnp.concatenate([st_t[0:1]] * 4 + [st_t[64:65]] * 4, axis=0)
    wo = jnp.concatenate([wo0_ref[0], wo1_ref[0]], axis=0)
    part = jnp.dot(o_ref[...], wo, preferred_element_type=F32)

    @pl.when(pl.program_id(0) == 0)
    def _():
        acc_ref[...] = part

    @pl.when(pl.program_id(0) > 0)
    def _():
        acc_ref[...] += part


def attn_fwd(h1, w0, w1, bias, cos_tab, sin_tab, mask_col, wo0, wo1):
    seq, dim = h1.shape
    heads = w0.shape[1] // 64
    full = lambda i: (0, 0)
    pair = pl.BlockSpec((seq, 128), lambda i: (0, i))
    head_w = pl.BlockSpec((3, 64, dim), lambda i: (0, i, 0))
    head_o = pl.BlockSpec((1, 64, dim), lambda i: (i, 0, 0))
    act = jax.ShapeDtypeStruct((seq, heads * 128), BF16)
    return pl.pallas_call(
        attn_fwd_kernel,
        grid=(heads,),
        in_specs=[pl.BlockSpec((seq, dim), full), head_w, head_w, pl.BlockSpec((1, 3, 128), lambda i: (i, 0, 0)),
                  pl.BlockSpec((seq, 128), full), pl.BlockSpec((seq, 128), full), pl.BlockSpec((seq, 128), full), head_o, head_o],
        out_specs=[pair, pair, pair, pair, pl.BlockSpec((1, 8, seq), lambda i: (i, 0, 0)), pl.BlockSpec((seq, dim), full)],
        out_shape=[act, act, act, act, jax.ShapeDtypeStruct((heads, 8, seq), F32), jax.ShapeDtypeStruct((seq, dim), F32)],
        scratch_shapes=[pltpu.VMEM((2, seq, 128), BF16), pltpu.VMEM((2, seq, 128), BF16), pltpu.VMEM((seq, 128), F32)],
        compiler_params=pltpu.CompilerParams(dimension_semantics=("arbitrary",), vmem_limit_bytes=VMEM_LIMIT),
        cost_estimate=pl.CostEstimate(flops=heads * 2 * seq * (dim * 512 + 4 * seq * 256), bytes_accessed=20_000_000, transcendentals=0),
        name="attn_fwd",
    )(h1, w0, w1, bias, cos_tab, sin_tab, mask_col, wo0, wo1)


def attn_bwd_kernel(h_ref, dx_ref, w0_ref, w1_ref, wo0_ref, wo1_ref, q_ref, k_ref, v_ref, o_ref, lse_ref, cos_ref, sin_ref, mb_ref,
                    dh_ref, gw0_ref, gw1_ref, gwo0_ref, gwo1_ref, gb_ref, qs, qz, ks, dos, kt, dqt, dk_acc, dv_acc):
    seq, _ = h_ref.shape
    lane = lax.broadcasted_iota(jnp.int32, (1, 128), 1)
    first_half = (lane % 64) < 32
    head0 = lane < 64
    dx = dx_ref[...]
    wo = jnp.concatenate([wo0_ref[0], wo1_ref[0]], axis=0)
    d_o = lax.dot_general(dx, wo, NT, preferred_element_type=F32)
    dos[0] = jnp.where(head0, d_o, 0.0).astype(BF16)
    dos[1] = jnp.where(head0, 0.0, d_o).astype(BF16)
    gwo = jnp.dot(o_ref[...].T, dx, preferred_element_type=F32)
    gwo0_ref[0] = gwo[:64]
    gwo1_ref[0] = gwo[64:]
    q, k, mb = q_ref[...].astype(F32), k_ref[...].astype(F32), mb_ref[...]
    qs[0] = jnp.where(head0, q, jnp.where(lane == 64, 1.0, 0.0)).astype(BF16)
    qs[1] = jnp.where(head0, jnp.where(lane == 0, 1.0, 0.0), q).astype(BF16)
    qz[0] = jnp.where(head0, q, 0.0).astype(BF16)
    qz[1] = jnp.where(head0, 0.0, q).astype(BF16)
    ks[0] = jnp.where(head0, k, jnp.where(lane == 64, mb, 0.0)).astype(BF16)
    ks[1] = jnp.where(head0, jnp.where(lane == 0, mb, 0.0), k).astype(BF16)
    kt[...] = k_ref[...].T
    dk_acc[...] = jnp.zeros_like(dk_acc)
    dv_acc[...] = jnp.zeros_like(dv_acc)

    def block(j, carry):
        rows = pl.ds(pl.multiple_of(j * QB, QB), QB)
        for head in range(2):
            s_t = lax.dot_general(ks[head], qs[head, rows, :], NT, preferred_element_type=F32)
            p_t = jnp.exp(s_t - lse_ref[0, 4 * head:4 * head + 1, rows])
            do_b = dos[head, rows, :]
            dp_t = lax.dot_general(v_ref[...], do_b, NT, preferred_element_type=F32)
            corr = jnp.sum(p_t * dp_t, axis=0, keepdims=True)
            ds_t = (p_t * (dp_t - corr)).astype(BF16)
            dv_acc[...] += jnp.dot(p_t.astype(BF16), do_b, preferred_element_type=F32)
            dk_acc[...] += jnp.dot(ds_t, qz[head, rows, :], preferred_element_type=F32)
            dqt[64 * head:64 * head + 64, rows] = jnp.dot(kt[64 * head:64 * head + 64, :], ds_t, preferred_element_type=F32)
        return carry

    lax.fori_loop(0, seq // QB, block, 0)
    cos, sin = cos_ref[...], sin_ref[...]
    dq, dk, dv = dqt[...].T, dk_acc[...], dv_acc[...]
    dq = (dq * cos - swap_halves(dq, first_half) * sin) * 0.125
    dk = dk * cos - swap_halves(dk, first_half) * sin
    d_all = jnp.concatenate([dq, dk, dv], axis=1)
    sums = jnp.sum(d_all, axis=0, keepdims=True)
    gb_ref[0] = jnp.concatenate([sums[:, :128], sums[:, 128:256], sums[:, 256:], jnp.zeros((5, 128), F32)], axis=0)
    d_low = d_all.astype(BF16)
    w = pair_rows(w0_ref, w1_ref)
    part = jnp.dot(d_low, w, preferred_element_type=F32)
    gw = jnp.dot(d_low.T, h_ref[...], preferred_element_type=F32)
    for i in range(3):
        gw0_ref[i] = gw[128 * i:128 * i + 64]
        gw1_ref[i] = gw[128 * i + 64:128 * i + 128]

    @pl.when(pl.program_id(0) == 0)
    def _():
        dh_ref[...] = part

    @pl.when(pl.program_id(0) > 0)
    def _():
        dh_ref[...] += part


def attn_bwd(h1, d_x1, w0, w1, wo0, wo1, q, k, v, o, lse, cos_tab, sin_tab, mask_col):
    seq, dim = h1.shape
    heads = w0.shape[1] // 64
    full = lambda i: (0, 0)
    pair = pl.BlockSpec((seq, 128), lambda i: (0, i))
    head_w = pl.BlockSpec((3, 64, dim), lambda i: (0, i, 0))
    head_o = pl.BlockSpec((1, 64, dim), lambda i: (i, 0, 0))
    tab = pl.BlockSpec((seq, 128), full)
    gw = jax.ShapeDtypeStruct((3, heads * 64, dim), F32)
    gwo = jax.ShapeDtypeStruct((heads, 64, dim), F32)
    half = pltpu.VMEM((2, seq, 128), BF16)
    return pl.pallas_call(
        attn_bwd_kernel,
        grid=(heads,),
        in_specs=[pl.BlockSpec((seq, dim), full), pl.BlockSpec((seq, dim), full), head_w, head_w, head_o, head_o, pair, pair, pair, pair,
                  pl.BlockSpec((1, 8, seq), lambda i: (i, 0, 0)), tab, tab, tab],
        out_specs=[pl.BlockSpec((seq, dim), full), head_w, head_w, head_o, head_o, pl.BlockSpec((1, 8, 128), lambda i: (i, 0, 0))],
        out_shape=[jax.ShapeDtypeStruct((seq, dim), F32), gw, gw, gwo, gwo, jax.ShapeDtypeStruct((heads, 8, 128), F32)],
        scratch_shapes=[half, half, half, half, pltpu.VMEM((128, seq), BF16), pltpu.VMEM((128, seq), F32),
                        pltpu.VMEM((seq, 128), F32), pltpu.VMEM((seq, 128), F32)],
        compiler_params=pltpu.CompilerParams(dimension_semantics=("arbitrary",), vmem_limit_bytes=VMEM_LIMIT),
        cost_estimate=pl.CostEstimate(flops=heads * 2 * seq * (dim * 1024 + 10 * seq * 256), bytes_accessed=40_000_000, transcendentals=0),
        name="attn_bwd",
    )(h1, d_x1, w0, w1, wo0, wo1, q, k, v, o, lse, cos_tab, sin_tab, mask_col)


def gelu_terms(pre):
    erf_term = lax.erf(pre * INV_SQRT2)
    act = 0.5 * pre * (1.0 + erf_term)
    slope = 0.5 * (1.0 + erf_term) + pre * jnp.exp(-0.5 * pre * pre) * INV_SQRT_2PI
    return act, slope


def mlp_kernel(tiles, n_w, *refs):
    h_ref, dy_ref, b_ref = refs[:3]
    up_refs, down_refs = refs[3:3 + n_w], refs[3 + n_w:3 + 2 * n_w]
    y_ref, dh_ref, wu, wd, sem = refs[3 + 2 * n_w:]
    seq = h_ref.shape[0]
    width = wu.shape[2]
    copies = []
    for t, (src, part) in enumerate(tiles):
        cols = pl.ds(part * width, width)
        copies.append((pltpu.make_async_copy(up_refs[src].at[:, cols], wu.at[t], sem.at[0, t]),
                       pltpu.make_async_copy(down_refs[src].at[cols, :], wd.at[t], sem.at[1, t])))
    for pair in copies:
        pair[0].start()
        pair[1].start()
    for t in range(len(tiles)):
        copies[t][0].wait()
        copies[t][1].wait()

        def block(j, carry, t=t):
            rows = pl.ds(pl.multiple_of(j * QB, QB), QB)
            pre = jnp.dot(h_ref[rows, :], wu[t], preferred_element_type=F32) + b_ref[t]
            act, slope = gelu_terms(pre)
            d_act = lax.dot_general(dy_ref[rows, :], wd[t], NT, preferred_element_type=F32)
            y_part = jnp.dot(act.astype(BF16), wd[t], preferred_element_type=F32)
            d_pre = (d_act * slope).astype(BF16)
            dh_part = lax.dot_general(d_pre, wu[t], NT, preferred_element_type=F32)
            if t == 0:
                y_ref[rows, :] = y_part
                dh_ref[rows, :] = dh_part
            else:
                y_ref[rows, :] += y_part
                dh_ref[rows, :] += dh_part
            return carry

        lax.fori_loop(0, seq // QB, block, 0)


def mlp_chain(h2, d_y, bias, ups, downs):
    seq, dim = h2.shape
    width = 640
    tiles = [(i, p) for i, w in enumerate(ups) for p in range(w.shape[1] // width)]
    vmem, hbm = pl.BlockSpec(memory_space=pltpu.VMEM), pl.BlockSpec(memory_space=pl.ANY)
    out = jax.ShapeDtypeStruct((seq, dim), F32)
    return pl.pallas_call(
        functools.partial(mlp_kernel, tiles, len(ups)),
        in_specs=[vmem, vmem, vmem] + [hbm] * (2 * len(ups)),
        out_specs=[vmem, vmem],
        out_shape=[out, out],
        scratch_shapes=[pltpu.VMEM((len(tiles), dim, width), BF16), pltpu.VMEM((len(tiles), width, dim), BF16),
                        pltpu.SemaphoreType.DMA((2, len(tiles)))],
        compiler_params=pltpu.CompilerParams(vmem_limit_bytes=VMEM_LIMIT),
        cost_estimate=pl.CostEstimate(flops=len(tiles) * 8 * seq * dim * width, bytes_accessed=30_000_000, transcendentals=0),
        name="mlp_chain",
    )(h2, d_y, bias.reshape(len(tiles), 1, width), *ups, *downs)


def xor_move(value, bits):
    return lax.ppermute(value, 'tp', [(i, i ^ bits) for i in range(4)])


def swap_groups(value):
    return lax.ppermute(value, 'dp', [(0, 1), (1, 0)])


def after(value, *others):
    return lax.optimization_barrier((value,) + others)[0]


def solution(mesh):
    act_spec = P('dp', 'tp', None)
    rep_vec = P(None)
    part_vec = P('dp')
    in_specs = (act_spec, act_spec, P('dp', None), rep_vec, rep_vec, P(None, None, 'tp', None), P(None, 'tp', None),
                P('tp', None, None), rep_vec, rep_vec, rep_vec, P(None, 'tp'), P('tp'), P('tp', None), rep_vec)
    out_specs = (act_spec, act_spec, part_vec, part_vec, P('dp', None, 'tp', None), P('dp', 'tp', None),
                 P(('dp', 'tp'), None, None), part_vec, part_vec, part_vec, P('dp', 'tp'), P(('dp', 'tp')),
                 P(('dp', 'tp'), None), part_vec)

    def layer(x_in, grad_y, pad_mask, ln1_gain, ln1_bias, w_qkv, b_qkv, w_out, b_out, ln2_gain, ln2_bias, w_up, b_up, w_down, b_down):
        me = lax.axis_index('tp')
        group = lax.axis_index('dp')
        core, far_chip = me % 2, 1 - me // 2
        n_seq, rows, dim = x_in.shape
        seq = pad_mask.shape[1]
        heads = w_out.shape[0]
        cols = w_up.shape[1]
        half = cols // 2

        def to_blocks(value):
            out = jnp.zeros((n_seq, rows, dim), value.dtype)
            for s in (0, 2, 3, 1):
                mine = lax.dynamic_slice_in_dim(value, (me ^ s) * rows, rows, 0)
                got = xor_move(mine, s) if s else mine
                out = lax.dynamic_update_index_in_dim(out, got, me ^ s, 0)
            return out

        x_seq = jnp.zeros((seq, dim), x_in.dtype)
        for s in (0, 1, 2, 3):
            mine = lax.dynamic_index_in_dim(x_in, me ^ s, 0, keepdims=False)
            got = xor_move(mine, s) if s else mine
            x_seq = lax.dynamic_update_slice_in_dim(x_seq, got, (me ^ s) * rows, 0)
        cos_tab, sin_tab = rope_tables(seq, 64)
        small = jnp.concatenate([b_up, b_qkv.reshape(-1)])
        smalls = [small] + [xor_move(small, s) for s in (1, 2, 3)]
        b_ups = [v[:cols] for v in smalls]
        b_qkvs = [v[cols:].reshape(3, heads, 64) for v in smalls]
        w_heads = jnp.transpose(w_qkv, (0, 2, 3, 1)).reshape(3, heads * 64, dim)
        wq = [w_heads, xor_move(w_heads, 1), xor_move(w_heads, 2)]
        wo = [w_out, xor_move(w_out, 1), xor_move(w_out, 2)]
        dy_far_part = xor_move(lax.dynamic_slice_in_dim(grad_y, far_chip * 2, 2, 0), 2)
        dy_next = xor_move(grad_y, 1)
        up2 = xor_move(lax.dynamic_slice_in_dim(w_up, group * half, half, 1), 2)
        down2 = xor_move(lax.dynamic_slice_in_dim(w_down, group * half, half, 0), 2)
        ups = [w_up, xor_move(w_up, 1)]
        downs = [w_down, xor_move(w_down, 1)]

        def ordered_bias(v):
            return jnp.where(group == 0, v, jnp.concatenate([v[half:], v[:half]]))

        my_mask = lax.dynamic_index_in_dim(pad_mask, me, 0, keepdims=False)
        mask_col = jnp.broadcast_to(jnp.where(my_mask > 0, 0.0, NEG_LARGE).astype(F32)[:, None], (seq, 128))
        x_f = x_seq.astype(F32)
        h1_f, x_hat1, inv_std1 = layer_norm(x_f, ln1_gain, ln1_bias)
        h1 = h1_f.astype(BF16)

        def pair_bias(a, b):
            return jnp.transpose(jnp.concatenate([a, b], axis=-1), (1, 0, 2))

        fwd_a = attn_fwd(h1, wq[0], wq[1], pair_bias(b_qkvs[0], b_qkvs[1]), cos_tab, sin_tab, mask_col, wo[0], wo[1])
        wq.append(xor_move(wq[2], 1))
        wo.append(xor_move(wo[2], 1))
        fwd_b = attn_fwd(h1, wq[2], wq[3], pair_bias(b_qkvs[2], b_qkvs[3]), cos_tab, sin_tab, mask_col, wo[2], wo[3])

        def chip_rows(own, beside, across, diagonal):
            out = jnp.zeros((2, seq, dim), own.dtype)
            for s, value in enumerate((own, beside, across, diagonal)):
                out = lax.dynamic_update_slice_in_dim(out, value, (me ^ s) * rows, 1)
            return out

        near = lambda v: lax.dynamic_slice_in_dim(v, (1 - far_chip) * 2, 2, 0)
        far = lambda v: lax.dynamic_slice_in_dim(v, far_chip * 2, 2, 0)
        dy_near = chip_rows(near(grad_y), near(dy_next), dy_far_part, xor_move(dy_far_part, 1))
        d_y = lax.dynamic_index_in_dim(dy_near, core, 0, keepdims=False)
        dy_f = d_y.astype(F32)
        x1_f = (x_f + ((fwd_a[5] + fwd_b[5]) + b_out)).astype(BF16).astype(F32)
        h2_f, x_hat2, inv_std2 = layer_norm(x1_f, ln2_gain, ln2_bias)
        h2 = h2_f.astype(BF16)
        h2_next = xor_move(h2, 1)
        h2_far = xor_move(after(h2, up2, down2), 2)
        dy_far_rest = xor_move(after(near(grad_y), up2, down2), 2)

        def by_core(mine, other):
            out = jnp.zeros((2, seq, dim), mine.dtype)
            out = lax.dynamic_update_index_in_dim(out, mine, core, 0)
            return lax.dynamic_update_index_in_dim(out, other, 1 - core, 0)

        def mlp_weight_grads(h2_two, dy_two):
            pre_act = jnp.einsum('bsd,df->bsf', h2_two, w_up, preferred_element_type=F32) + b_up
            act, gelu_slope = gelu_terms(pre_act)
            g_down = jnp.einsum('bsf,bsd->fd', act.astype(BF16), dy_two, preferred_element_type=F32)
            d_act = jnp.einsum('bsd,fd->bsf', dy_two, w_down, preferred_element_type=F32)
            d_pre = d_act * gelu_slope
            g_up = jnp.einsum('bsd,bsf->df', h2_two, d_pre.astype(BF16), preferred_element_type=F32)
            return g_up, g_down, jnp.sum(d_pre, axis=(0, 1))

        y_a, dh2_a = mlp_chain(h2, d_y, jnp.concatenate([b_ups[0], b_ups[1]]), ups, downs)
        ups_far = [up2, swap_groups(after(up2, y_a))]
        downs_far = [down2, swap_groups(after(down2, y_a))]
        near_grads = mlp_weight_grads(by_core(after(h2, y_a), h2_next), dy_near)
        ups_far += [xor_move(after(v, *near_grads), 1) for v in ups_far]
        downs_far += [xor_move(after(v, *near_grads), 1) for v in downs_far]
        y_b, dh2_b = mlp_chain(h2, d_y, jnp.concatenate([ordered_bias(b_ups[2]), ordered_bias(b_ups[3])]), ups_far, downs_far)
        y_seq = (x1_f + ((y_a + y_b) + b_down)).astype(BF16)
        y_out = to_blocks(y_seq)
        d_h2 = dh2_a + dh2_b
        d_x1 = dy_f + layer_norm_grad(d_h2, x_hat2, inv_std2, ln2_gain)
        d_x1_b = d_x1.astype(BF16)

        def backward(i, fwd, d_mid):
            q, k, v, o, lse, _ = fwd
            return attn_bwd(h1, d_mid, wq[i], wq[i + 1], wo[i], wo[i + 1], q, k, v, o, lse, cos_tab, sin_tab, mask_col)

        bwd_b = backward(2, fwd_b, d_x1_b)
        gq_far = bwd_b[1] + xor_move(bwd_b[2], 1)
        go_far = bwd_b[3] + xor_move(bwd_b[4], 1)
        gq_across = xor_move(gq_far, 2)
        go_across = xor_move(go_far, 2)
        bwd_a = backward(0, fwd_a, after(d_x1_b, gq_far, go_far))
        d_h1 = bwd_b[0] + bwd_a[0]
        grad_x_seq = (d_x1 + layer_norm_grad(d_h1, x_hat1, inv_std1, ln1_gain)).astype(BF16)
        grad_x = to_blocks(grad_x_seq)
        grads_q = (bwd_a[1] + xor_move(bwd_a[2], 1)) + gq_across
        grad_w_qkv = jnp.transpose(grads_q.reshape(3, heads, 64, dim), (0, 3, 1, 2))
        grad_w_out = (bwd_a[3] + xor_move(bwd_a[4], 1)) + go_across
        gb = []
        for part in (bwd_a[5], bwd_b[5]):
            part = jnp.transpose(part[:, :3], (1, 0, 2))
            gb += [part[..., :64], part[..., 64:]]
        grad_b_qkv = (gb[0] + xor_move(gb[1], 1)) + (xor_move(gb[2], 2) + xor_move(gb[3], 3))

        dy_far = chip_rows(far(grad_y), far(dy_next), dy_far_rest, xor_move(after(dy_far_rest, bwd_b[0]), 1))
        h2_far_next = xor_move(after(h2_far, bwd_b[0]), 1)
        far_grads = mlp_weight_grads(by_core(after(h2_far, grad_x_seq), h2_far_next), dy_far)
        grad_w_up, grad_w_down, grad_b_up = (a + b for a, b in zip(near_grads, far_grads))

        sums = jnp.stack([jnp.sum(dy_f, axis=0), jnp.sum(d_h2 * x_hat2, axis=0), jnp.sum(d_h2, axis=0), jnp.sum(d_x1, axis=0),
                          jnp.sum(d_h1 * x_hat1, axis=0), jnp.sum(d_h1, axis=0)])
        sums = sums + xor_move(sums, 1)
        sums = sums + xor_move(sums, 2)
        return (y_out, grad_x, sums[4], sums[5], grad_w_qkv, grad_b_qkv, grad_w_out, sums[3],
                sums[1], sums[2], grad_w_up, grad_b_up, grad_w_down, sums[0])

    return jax.shard_map(layer, mesh=mesh, in_specs=in_specs, out_specs=out_specs, check_vma=False)
```

```python
import functools

import jax
import jax.numpy as jnp
from jax import lax
from jax.experimental import pallas as pl
from jax.experimental.pallas import tpu as pltpu
from jax.sharding import PartitionSpec as P


LN_EPS = 1e-5
ROPE_BASE = 10000.0
INV_SQRT2 = 0.7071067811865476
INV_SQRT_2PI = 0.3989422804014327
NEG_LARGE = -1e30
F32 = jnp.float32
BF16 = jnp.bfloat16
NT = (((1,), (1,)), ((), ()))
VMEM_LIMIT = 60 * 1024 * 1024
QB = 256


def layer_norm(values, ln_gain, ln_bias):
    centered = values - jnp.mean(values, axis=-1, keepdims=True)
    inv_std = lax.rsqrt(jnp.mean(centered * centered, axis=-1, keepdims=True) + LN_EPS)
    x_hat = centered * inv_std
    return x_hat * ln_gain + ln_bias, x_hat, inv_std


def layer_norm_grad(d_out, x_hat, inv_std, ln_gain):
    d_hat = d_out * ln_gain
    return inv_std * (d_hat - jnp.mean(d_hat, axis=-1, keepdims=True) - x_hat * jnp.mean(d_hat * x_hat, axis=-1, keepdims=True))


def rope_tables(positions, head_dim):
    half_dim = head_dim // 2
    inv_freq = ROPE_BASE ** (-2.0 * jnp.arange(half_dim, dtype=F32) / head_dim)
    angles = positions.astype(F32)[:, None] * inv_freq[None, :]
    cos_half, sin_half = jnp.cos(angles), jnp.sin(angles)
    cos_tab = jnp.concatenate([cos_half] * 4, axis=-1)
    sin_tab = jnp.concatenate([-sin_half, sin_half, -sin_half, sin_half], axis=-1)
    return cos_tab, sin_tab


def swap_halves(t, first_half):
    return jnp.where(first_half, pltpu.roll(t, 96, 1), pltpu.roll(t, 32, 1))


def pair_rows(ref0, ref1):
    return jnp.concatenate([r[i] for i in range(3) for r in (ref0, ref1)], axis=0)


def attn_fwd_kernel(h_ref, w0_ref, w1_ref, b_ref, cos_ref, sin_ref, mb_ref, wo0_ref, wo1_ref,
                    q_ref, k_ref, v_ref, o_ref, lse_ref, acc_ref, qs, ks, st):
    seq = h_ref.shape[0]
    lane = lax.broadcasted_iota(jnp.int32, (1, 128), 1)
    first_half = (lane % 64) < 32
    head0 = lane < 64
    w = pair_rows(w0_ref, w1_ref)
    t = lax.dot_general(h_ref[...], w, NT, preferred_element_type=F32)
    cos, sin = cos_ref[...], sin_ref[...]
    tq = (t[:, :128] + b_ref[0, 0:1]) * 0.125
    tk = t[:, 128:256] + b_ref[0, 1:2]
    q = (tq * cos + swap_halves(tq, first_half) * sin).astype(BF16)
    k = (tk * cos + swap_halves(tk, first_half) * sin).astype(BF16)
    v_ref[...] = (t[:, 256:] + b_ref[0, 2:3]).astype(BF16)
    q_ref[...] = q
    k_ref[...] = k
    q, k = q.astype(F32), k.astype(F32)
    mb = mb_ref[...]
    qs[0] = jnp.where(head0, q, jnp.where(lane == 64, 1.0, 0.0)).astype(BF16)
    qs[1] = jnp.where(head0, jnp.where(lane == 0, 1.0, 0.0), q).astype(BF16)
    ks[0] = jnp.where(head0, k, jnp.where(lane == 64, mb, 0.0)).astype(BF16)
    ks[1] = jnp.where(head0, jnp.where(lane == 0, mb, 0.0), k).astype(BF16)

    def block(j, carry):
        rows = pl.ds(pl.multiple_of(j * QB, QB), QB)
        outs, stats = [], []
        for head in range(2):
            s = lax.dot_general(qs[head, rows, :], ks[head], NT, preferred_element_type=F32)
            m = jnp.max(s, axis=-1, keepdims=True)
            e = jnp.exp(s - m)
            total = jnp.sum(e, axis=-1, keepdims=True)
            p = (e * (1.0 / total)).astype(BF16)
            outs.append(jnp.dot(p, v_ref[...], preferred_element_type=F32))
            stats.append(m + jnp.log(total))
        o_ref[rows, :] = jnp.where(head0, outs[0], outs[1]).astype(BF16)
        st[rows, :] = jnp.where(head0, stats[0], stats[1])
        return carry

    lax.fori_loop(0, seq // QB, block, 0)
    st_t = st[...].T
    lse_ref[0] = jnp.concatenate([st_t[0:1]] * 4 + [st_t[64:65]] * 4, axis=0)
    wo = jnp.concatenate([wo0_ref[0], wo1_ref[0]], axis=0)
    part = jnp.dot(o_ref[...], wo, preferred_element_type=F32)

    @pl.when(pl.program_id(0) == 0)
    def _():
        acc_ref[...] = part

    @pl.when(pl.program_id(0) > 0)
    def _():
        acc_ref[...] += part


def attn_fwd(h1, w0, w1, bias, cos_tab, sin_tab, mask_col, wo0, wo1):
    seq, dim = h1.shape
    heads = w0.shape[1] // 64
    full = lambda i: (0, 0)
    pair = pl.BlockSpec((seq, 128), lambda i: (0, i))
    head_w = pl.BlockSpec((3, 64, dim), lambda i: (0, i, 0))
    head_o = pl.BlockSpec((1, 64, dim), lambda i: (i, 0, 0))
    act = jax.ShapeDtypeStruct((seq, heads * 128), BF16)
    return pl.pallas_call(
        attn_fwd_kernel,
        grid=(heads,),
        in_specs=[pl.BlockSpec((seq, dim), full), head_w, head_w, pl.BlockSpec((1, 3, 128), lambda i: (i, 0, 0)),
                  pl.BlockSpec((seq, 128), full), pl.BlockSpec((seq, 128), full), pl.BlockSpec((seq, 128), full), head_o, head_o],
        out_specs=[pair, pair, pair, pair, pl.BlockSpec((1, 8, seq), lambda i: (i, 0, 0)), pl.BlockSpec((seq, dim), full)],
        out_shape=[act, act, act, act, jax.ShapeDtypeStruct((heads, 8, seq), F32), jax.ShapeDtypeStruct((seq, dim), F32)],
        scratch_shapes=[pltpu.VMEM((2, seq, 128), BF16), pltpu.VMEM((2, seq, 128), BF16), pltpu.VMEM((seq, 128), F32)],
        compiler_params=pltpu.CompilerParams(dimension_semantics=("arbitrary",), vmem_limit_bytes=VMEM_LIMIT),
        cost_estimate=pl.CostEstimate(flops=heads * 2 * seq * (dim * 512 + 4 * seq * 256), bytes_accessed=20_000_000, transcendentals=0),
        name="attn_fwd",
    )(h1, w0, w1, bias, cos_tab, sin_tab, mask_col, wo0, wo1)


def attn_bwd_kernel(h_ref, dx_ref, w0_ref, w1_ref, wo0_ref, wo1_ref, q_ref, k_ref, v_ref, o_ref, lse_ref, cos_ref, sin_ref, mb_ref,
                    dh_ref, gw0_ref, gw1_ref, gb_ref, qs, qz, ks, dos, kt, dqt, dk_acc, dv_acc):
    seq, _ = h_ref.shape
    lane = lax.broadcasted_iota(jnp.int32, (1, 128), 1)
    first_half = (lane % 64) < 32
    head0 = lane < 64
    dx = dx_ref[...]
    wo = jnp.concatenate([wo0_ref[0], wo1_ref[0]], axis=0)
    d_o = lax.dot_general(dx, wo, NT, preferred_element_type=F32)
    dos[0] = jnp.where(head0, d_o, 0.0).astype(BF16)
    dos[1] = jnp.where(head0, 0.0, d_o).astype(BF16)
    gwo = jnp.dot(o_ref[...].T, dx, preferred_element_type=F32)
    gw0_ref[3] = gwo[:64]
    gw1_ref[3] = gwo[64:]
    q, k, mb = q_ref[...].astype(F32), k_ref[...].astype(F32), mb_ref[...]
    qs[0] = jnp.where(head0, q, jnp.where(lane == 64, 1.0, 0.0)).astype(BF16)
    qs[1] = jnp.where(head0, jnp.where(lane == 0, 1.0, 0.0), q).astype(BF16)
    qz[0] = jnp.where(head0, q, 0.0).astype(BF16)
    qz[1] = jnp.where(head0, 0.0, q).astype(BF16)
    ks[0] = jnp.where(head0, k, jnp.where(lane == 64, mb, 0.0)).astype(BF16)
    ks[1] = jnp.where(head0, jnp.where(lane == 0, mb, 0.0), k).astype(BF16)
    kt[...] = k_ref[...].T
    dk_acc[...] = jnp.zeros_like(dk_acc)
    dv_acc[...] = jnp.zeros_like(dv_acc)

    def block(j, carry):
        rows = pl.ds(pl.multiple_of(j * QB, QB), QB)
        for head in range(2):
            s_t = lax.dot_general(ks[head], qs[head, rows, :], NT, preferred_element_type=F32)
            p_t = jnp.exp(s_t - lse_ref[0, 4 * head:4 * head + 1, rows])
            do_b = dos[head, rows, :]
            dp_t = lax.dot_general(v_ref[...], do_b, NT, preferred_element_type=F32)
            corr = jnp.sum(p_t * dp_t, axis=0, keepdims=True)
            ds_t = (p_t * (dp_t - corr)).astype(BF16)
            dv_acc[...] += jnp.dot(p_t.astype(BF16), do_b, preferred_element_type=F32)
            dk_acc[...] += jnp.dot(ds_t, qz[head, rows, :], preferred_element_type=F32)
            dqt[64 * head:64 * head + 64, rows] = jnp.dot(kt[64 * head:64 * head + 64, :], ds_t, preferred_element_type=F32)
        return carry

    lax.fori_loop(0, seq // QB, block, 0)
    cos, sin = cos_ref[...], sin_ref[...]
    dq, dk, dv = dqt[...].T, dk_acc[...], dv_acc[...]
    dq = (dq * cos - swap_halves(dq, first_half) * sin) * 0.125
    dk = dk * cos - swap_halves(dk, first_half) * sin
    d_all = jnp.concatenate([dq, dk, dv], axis=1)
    sums = jnp.sum(d_all, axis=0, keepdims=True)
    gb_ref[0] = jnp.concatenate([sums[:, :128], sums[:, 128:256], sums[:, 256:], jnp.zeros((5, 128), F32)], axis=0)
    d_low = d_all.astype(BF16)
    w = pair_rows(w0_ref, w1_ref)
    part = jnp.dot(d_low, w, preferred_element_type=F32)
    gw = jnp.dot(d_low.T, h_ref[...], preferred_element_type=F32)
    for i in range(3):
        gw0_ref[i] = gw[128 * i:128 * i + 64]
        gw1_ref[i] = gw[128 * i + 64:128 * i + 128]

    @pl.when(pl.program_id(0) == 0)
    def _():
        dh_ref[...] = part

    @pl.when(pl.program_id(0) > 0)
    def _():
        dh_ref[...] += part


def attn_bwd(h1, d_x1, w0, w1, wo0, wo1, q, k, v, o, lse, cos_tab, sin_tab, mask_col):
    seq, dim = h1.shape
    heads = w0.shape[1] // 64
    full = lambda i: (0, 0)
    pair = pl.BlockSpec((seq, 128), lambda i: (0, i))
    head_w = pl.BlockSpec((3, 64, dim), lambda i: (0, i, 0))
    head_o = pl.BlockSpec((1, 64, dim), lambda i: (i, 0, 0))
    tab = pl.BlockSpec((seq, 128), full)
    gw = jax.ShapeDtypeStruct((4, heads * 64, dim), F32)
    head_g = pl.BlockSpec((4, 64, dim), lambda i: (0, i, 0))
    half = pltpu.VMEM((2, seq, 128), BF16)
    return pl.pallas_call(
        attn_bwd_kernel,
        grid=(heads,),
        in_specs=[pl.BlockSpec((seq, dim), full), pl.BlockSpec((seq, dim), full), head_w, head_w, head_o, head_o, pair, pair, pair, pair,
                  pl.BlockSpec((1, 8, seq), lambda i: (i, 0, 0)), tab, tab, tab],
        out_specs=[pl.BlockSpec((seq, dim), full), head_g, head_g, pl.BlockSpec((1, 8, 128), lambda i: (i, 0, 0))],
        out_shape=[jax.ShapeDtypeStruct((seq, dim), F32), gw, gw, jax.ShapeDtypeStruct((heads, 8, 128), F32)],
        scratch_shapes=[half, half, half, half, pltpu.VMEM((128, seq), BF16), pltpu.VMEM((128, seq), F32),
                        pltpu.VMEM((seq, 128), F32), pltpu.VMEM((seq, 128), F32)],
        compiler_params=pltpu.CompilerParams(dimension_semantics=("arbitrary",), vmem_limit_bytes=VMEM_LIMIT),
        cost_estimate=pl.CostEstimate(flops=heads * 2 * seq * (dim * 1024 + 10 * seq * 256), bytes_accessed=40_000_000, transcendentals=0),
        name="attn_bwd",
    )(h1, d_x1, w0, w1, wo0, wo1, q, k, v, o, lse, cos_tab, sin_tab, mask_col)


def gelu_terms(pre):
    erf_term = lax.erf(pre * INV_SQRT2)
    act = 0.5 * pre * (1.0 + erf_term)
    slope = 0.5 * (1.0 + erf_term) + pre * jnp.exp(-0.5 * pre * pre) * INV_SQRT_2PI
    return act, slope


def mlp_kernel(tiles, n_w, *refs):
    h_ref, dy_ref, b_ref = refs[:3]
    up_refs, down_refs = refs[3:3 + n_w], refs[3 + n_w:3 + 2 * n_w]
    y_ref, dh_ref, wu, wd, sem = refs[3 + 2 * n_w:]
    seq = h_ref.shape[0]
    width = wu.shape[2]
    copies = []
    for t, (src, part) in enumerate(tiles):
        cols = pl.ds(part * width, width)
        copies.append((pltpu.make_async_copy(up_refs[src].at[:, cols], wu.at[t], sem.at[0, t]),
                       pltpu.make_async_copy(down_refs[src].at[cols, :], wd.at[t], sem.at[1, t])))
    for pair in copies:
        pair[0].start()
        pair[1].start()
    for t in range(len(tiles)):
        copies[t][0].wait()
        copies[t][1].wait()

        def block(j, carry, t=t):
            rows = pl.ds(pl.multiple_of(j * QB, QB), QB)
            pre = jnp.dot(h_ref[rows, :], wu[t], preferred_element_type=F32) + b_ref[t]
            act, slope = gelu_terms(pre)
            d_act = lax.dot_general(dy_ref[rows, :], wd[t], NT, preferred_element_type=F32)
            y_part = jnp.dot(act.astype(BF16), wd[t], preferred_element_type=F32)
            d_pre = (d_act * slope).astype(BF16)
            dh_part = lax.dot_general(d_pre, wu[t], NT, preferred_element_type=F32)
            if t == 0:
                y_ref[rows, :] = y_part
                dh_ref[rows, :] = dh_part
            else:
                y_ref[rows, :] += y_part
                dh_ref[rows, :] += dh_part
            return carry

        lax.fori_loop(0, seq // QB, block, 0)


def mlp_chain(h2, d_y, bias, ups, downs):
    seq, dim = h2.shape
    width = 640
    tiles = [(i, p) for i, w in enumerate(ups) for p in range(w.shape[1] // width)]
    vmem, hbm = pl.BlockSpec(memory_space=pltpu.VMEM), pl.BlockSpec(memory_space=pl.ANY)
    out = jax.ShapeDtypeStruct((seq, dim), F32)
    return pl.pallas_call(
        functools.partial(mlp_kernel, tiles, len(ups)),
        in_specs=[vmem, vmem, vmem] + [hbm] * (2 * len(ups)),
        out_specs=[vmem, vmem],
        out_shape=[out, out],
        scratch_shapes=[pltpu.VMEM((len(tiles), dim, width), BF16), pltpu.VMEM((len(tiles), width, dim), BF16),
                        pltpu.SemaphoreType.DMA((2, len(tiles)))],
        compiler_params=pltpu.CompilerParams(vmem_limit_bytes=VMEM_LIMIT),
        cost_estimate=pl.CostEstimate(flops=len(tiles) * 8 * seq * dim * width, bytes_accessed=30_000_000, transcendentals=0),
        name="mlp_chain",
    )(h2, d_y, bias.reshape(len(tiles), 1, width), *ups, *downs)


def xor_move(value, bits):
    return lax.ppermute(value, 'tp', [(i, i ^ bits) for i in range(4)])


def swap_groups(value):
    return lax.ppermute(value, 'dp', [(0, 1), (1, 0)])


def after(value, *others):
    return lax.optimization_barrier((value,) + others)[0]


def solution(mesh):
    act_spec = P('dp', 'tp', None)
    rep_vec = P(None)
    part_vec = P('dp')
    in_specs = (act_spec, act_spec, P('dp', None), rep_vec, rep_vec, P(None, None, 'tp', None), P(None, 'tp', None),
                P('tp', None, None), rep_vec, rep_vec, rep_vec, P(None, 'tp'), P('tp'), P('tp', None), rep_vec)
    out_specs = (act_spec, act_spec, part_vec, part_vec, P('dp', None, 'tp', None), P('dp', 'tp', None),
                 P(('dp', 'tp'), None, None), part_vec, part_vec, part_vec, P('dp', 'tp'), P(('dp', 'tp')),
                 P(('dp', 'tp'), None), part_vec)

    def layer(x_in, grad_y, pad_mask, ln1_gain, ln1_bias, w_qkv, b_qkv, w_out, b_out, ln2_gain, ln2_bias, w_up, b_up, w_down, b_down):
        me = lax.axis_index('tp')
        group = lax.axis_index('dp')
        core, chip = me % 2, me // 2
        _, rows, dim = x_in.shape
        heads = w_out.shape[0]
        cols = w_up.shape[1]
        half = cols // 2

        def pick(blocks, index):
            return lax.dynamic_index_in_dim(blocks, index, 0, keepdims=False)

        def to_blocks(value):
            v = [value[s * rows:(s + 1) * rows] for s in range(4)]
            v = [v[0]] + [xor_move(v[s], s) for s in (1, 2, 3)]
            low = [jnp.where(core == 1, a, b) for a, b in ((v[1], v[0]), (v[0], v[1]))]
            high = [jnp.where(core == 1, a, b) for a, b in ((v[3], v[2]), (v[2], v[3]))]
            first = [jnp.where(chip == 1, b, a) for a, b in zip(low, high)]
            last = [jnp.where(chip == 1, a, b) for a, b in zip(low, high)]
            return jnp.stack(first + last)

        x_slots = [pick(x_in, me ^ s) for s in range(4)]
        x_seq = jnp.concatenate([x_slots[0]] + [xor_move(x_slots[s], s) for s in (1, 2, 3)])
        small = jnp.concatenate([b_up, jnp.transpose(b_qkv, (1, 0, 2)).reshape(-1)])
        smalls = [small] + [xor_move(small, s) for s in (1, 2, 3)]
        b_ups = [v[:cols].reshape(2, 1, half) for v in smalls]
        b_qkvs = [v[cols:].reshape(heads, 3, 64) for v in smalls]
        w_heads = jnp.transpose(w_qkv, (0, 2, 3, 1)).reshape(3, heads * 64, dim)
        wq = [w_heads, xor_move(w_heads, 1), xor_move(w_heads, 2)]
        wo = [w_out, xor_move(w_out, 1), xor_move(w_out, 2)]
        dya2 = xor_move(lax.dynamic_slice_in_dim(grad_y, (1 - chip) * 2, 2, 0), 2)
        dy1 = xor_move(grad_y, 1)
        up2 = xor_move(lax.dynamic_slice_in_dim(w_up, group * half, half, 1), 2)
        down2 = xor_move(lax.dynamic_slice_in_dim(w_down, group * half, half, 0), 2)
        ups = [w_up, xor_move(w_up, 1)]
        downs = [w_down, xor_move(w_down, 1)]

        positions = jnp.concatenate([(me ^ s) * rows + jnp.arange(rows) for s in range(4)])
        cos_tab, sin_tab = rope_tables(positions, 64)
        length = jnp.sum((pick(pad_mask, me) > 0).astype(jnp.int32))
        mask_col = jnp.broadcast_to(jnp.where(positions < length, 0.0, NEG_LARGE).astype(F32)[:, None], (4 * rows, 128))
        x_f = x_seq.astype(F32)
        h1_f, x_hat1, inv_std1 = layer_norm(x_f, ln1_gain, ln1_bias)
        h1 = h1_f.astype(BF16)

        def pair_bias(a, b):
            return jnp.concatenate([a, b], axis=-1)

        fwd_a = attn_fwd(h1, wq[0], wq[1], pair_bias(b_qkvs[0], b_qkvs[1]), cos_tab, sin_tab, mask_col, wo[0], wo[1])
        wq.append(xor_move(wq[2], 1))
        wo.append(xor_move(wo[2], 1))
        fwd_b = attn_fwd(h1, wq[2], wq[3], pair_bias(b_qkvs[2], b_qkvs[3]), cos_tab, sin_tab, mask_col, wo[2], wo[3])

        x1_f = (x_f + ((fwd_a[5] + fwd_b[5]) + b_out)).astype(BF16).astype(F32)
        h2_f, x_hat2, inv_std2 = layer_norm(x1_f, ln2_gain, ln2_bias)
        h2 = h2_f.astype(BF16)
        dya3 = xor_move(dya2, 1)
        h2_next = xor_move(h2, 1)
        d_y = jnp.concatenate([pick(grad_y, me), pick(dy1, me), pick(dya2, core), pick(dya3, core)])
        d_y_next = jnp.concatenate([pick(dy1, me ^ 1), pick(grad_y, me ^ 1), pick(dya3, 1 - core), pick(dya2, 1 - core)])
        dy_f = d_y.astype(F32)

        def up_part(h2_two):
            return jnp.dot(h2_two, w_up, preferred_element_type=F32) + b_up

        def mlp_weight_grads(h2_two, pre_act, dy_two):
            act, gelu_slope = gelu_terms(pre_act)
            g_down = jnp.einsum('sf,sd->fd', act.astype(BF16), dy_two, preferred_element_type=F32)
            d_act = jnp.einsum('sd,fd->sf', dy_two, w_down, preferred_element_type=F32)
            d_pre = d_act * gelu_slope
            g_up = jnp.einsum('sd,sf->df', h2_two, d_pre.astype(BF16), preferred_element_type=F32)
            return g_up, g_down, jnp.sum(d_pre, axis=0)

        h2_near = jnp.concatenate([h2, h2_next])
        pre_near = up_part(h2_near)

        up_y = swap_groups(after(up2, pre_near))
        y_a, dh2_a = mlp_chain(after(h2, pre_near), d_y, jnp.concatenate([b_ups[0], b_ups[1]]), ups, downs)
        down_y = swap_groups(after(down2, y_a))
        near_grads = mlp_weight_grads(h2_near, after(pre_near, y_a), jnp.concatenate([d_y, d_y_next]))
        h2_far = xor_move(after(h2, down2), 2)
        dyb2 = xor_move(after(lax.dynamic_slice_in_dim(grad_y, chip * 2, 2, 0), down2), 2)
        ups_far, downs_far = [up2, up_y], [down2, down_y]
        ups_far += [xor_move(after(v, y_a), 1) for v in ups_far]
        downs_far += [xor_move(after(v, near_grads[0]), 1) for v in downs_far]
        far_bias = [jnp.where(group == 0, v, v[::-1]) for v in b_ups[2:]]
        y_b, dh2_b = mlp_chain(after(h2, *near_grads), d_y, jnp.concatenate(far_bias), ups_far, downs_far)
        y_seq = (x1_f + ((y_a + y_b) + b_down)).astype(BF16)
        y_out = to_blocks(y_seq)
        d_h2 = dh2_a + dh2_b
        d_x1 = dy_f + layer_norm_grad(d_h2, x_hat2, inv_std2, ln2_gain)
        d_x1_b = d_x1.astype(BF16)

        def backward(i, fwd, d_mid):
            q, k, v, o, lse, _ = fwd
            return attn_bwd(h1, d_mid, wq[i], wq[i + 1], wo[i], wo[i + 1], q, k, v, o, lse, cos_tab, sin_tab, mask_col)

        bwd_b = backward(2, fwd_b, d_x1_b)
        g_far = bwd_b[1] + xor_move(bwd_b[2], 1)
        g_across = xor_move(g_far, 2)
        dyb3 = xor_move(after(dyb2, bwd_b[0]), 1)
        h2_far_next = xor_move(after(h2_far, bwd_b[0]), 1)
        bwd_a = backward(0, fwd_a, after(d_x1_b, g_far))
        d_h1 = bwd_b[0] + bwd_a[0]
        grad_x_seq = (d_x1 + layer_norm_grad(d_h1, x_hat1, inv_std1, ln1_gain)).astype(BF16)
        sums = jnp.concatenate([jnp.sum(v, axis=0) for v in (dy_f, d_h2 * x_hat2, d_h2, d_x1, d_h1 * x_hat1, d_h1)])
        gb = []
        for part in (bwd_a[3], bwd_b[3]):
            part = jnp.transpose(part[:, :3], (1, 0, 2))
            gb += [part[..., :64].reshape(-1), part[..., 64:].reshape(-1)]
        packs = [jnp.concatenate([sums, v]) for v in gb]
        packs = [packs[0]] + [xor_move(packs[s], s) for s in (1, 2, 3)]
        totals = (packs[0] + packs[1]) + (packs[2] + packs[3])
        sums, grad_b_qkv = totals[:6 * dim].reshape(6, dim), totals[6 * dim:].reshape(3, heads, 64)
        grad_x = to_blocks(grad_x_seq)
        g_all = (bwd_a[1] + xor_move(bwd_a[2], 1)) + g_across
        grad_w_qkv = jnp.transpose(g_all[:3].reshape(3, heads, 64, dim), (0, 3, 1, 2))
        grad_w_out = g_all[3].reshape(heads, 64, dim)

        dy_far = jnp.concatenate([pick(dyb2, core), pick(dyb3, core), pick(grad_y, me ^ 2), pick(dy1, me ^ 2),
                                  pick(dyb3, 1 - core), pick(dyb2, 1 - core), pick(dy1, me ^ 3), pick(grad_y, me ^ 3)])
        h2_other = jnp.concatenate([after(h2_far, grad_x_seq), h2_far_next])
        far_grads = mlp_weight_grads(h2_other, up_part(h2_other), dy_far)
        grad_w_up, grad_w_down, grad_b_up = (a + b for a, b in zip(near_grads, far_grads))
        return (y_out, grad_x, sums[4], sums[5], grad_w_qkv, grad_b_qkv, grad_w_out, sums[3],
                sums[1], sums[2], grad_w_up, grad_b_up, grad_w_down, sums[0])

    return jax.shard_map(layer, mesh=mesh, in_specs=in_specs, out_specs=out_specs, check_vma=False)
```

```python
import functools

import jax
import jax.numpy as jnp
from jax import lax
from jax.experimental import pallas as pl
from jax.experimental.pallas import tpu as pltpu
from jax.sharding import PartitionSpec as P


LN_EPS = 1e-5
ROPE_BASE = 10000.0
INV_SQRT2 = 0.7071067811865476
INV_SQRT_2PI = 0.3989422804014327
NEG_LARGE = -1e30
F32 = jnp.float32
BF16 = jnp.bfloat16
NT = (((1,), (1,)), ((), ()))
VMEM_LIMIT = 60 << 20
LANES = 128
HD = 64
QB = 256


def layer_norm(values, ln_gain, ln_bias):
    centered = values - jnp.mean(values, axis=-1, keepdims=True)
    inv_std = lax.rsqrt(jnp.mean(centered * centered, axis=-1, keepdims=True) + LN_EPS)
    x_hat = centered * inv_std
    return x_hat * ln_gain + ln_bias, x_hat, inv_std


def layer_norm_grad(d_out, x_hat, inv_std, ln_gain):
    d_hat = d_out * ln_gain
    return inv_std * (d_hat - jnp.mean(d_hat, axis=-1, keepdims=True) - x_hat * jnp.mean(d_hat * x_hat, axis=-1, keepdims=True))


def rope_tables(positions, head_dim):
    half_dim = head_dim // 2
    inv_freq = ROPE_BASE ** (-2.0 * jnp.arange(half_dim, dtype=F32) / head_dim)
    angles = positions.astype(F32)[:, None] * inv_freq[None, :]
    cos_half, sin_half = jnp.cos(angles), jnp.sin(angles)
    cos_tab = jnp.concatenate([cos_half] * 4, axis=-1)
    sin_tab = jnp.concatenate([-sin_half, sin_half, -sin_half, sin_half], axis=-1)
    return cos_tab, sin_tab


def swap_halves(t, first_half):
    return jnp.where(first_half, pltpu.roll(t, 96, 1), pltpu.roll(t, 32, 1))


def pair_rows(ref0, ref1):
    return jnp.concatenate([r[i] for i in range(3) for r in (ref0, ref1)], axis=0)


def attn_fwd_kernel(h_ref, w0_ref, w1_ref, b_ref, cos_ref, sin_ref, mb_ref, q_ref, k_ref, v_ref, o_ref, lse_ref, qs, ks, st):
    seq = h_ref.shape[0]
    lane = lax.broadcasted_iota(jnp.int32, (1, LANES), 1)
    first_half = (lane % HD) < 32
    head0 = lane < HD
    w = pair_rows(w0_ref, w1_ref)
    t = lax.dot_general(h_ref[...], w, NT, preferred_element_type=F32)
    cos, sin = cos_ref[...], sin_ref[...]
    tq = (t[:, :LANES] + b_ref[0, 0:1]) * 0.125
    tk = t[:, LANES:256] + b_ref[0, 1:2]
    q = (tq * cos + swap_halves(tq, first_half) * sin).astype(BF16)
    k = (tk * cos + swap_halves(tk, first_half) * sin).astype(BF16)
    v_ref[...] = (t[:, 256:] + b_ref[0, 2:3]).astype(BF16)
    q_ref[...] = q
    k_ref[...] = k
    q, k = q.astype(F32), k.astype(F32)
    mb = mb_ref[...]
    qs[0] = jnp.where(head0, q, jnp.where(lane == HD, 1.0, 0.0)).astype(BF16)
    qs[1] = jnp.where(head0, jnp.where(lane == 0, 1.0, 0.0), q).astype(BF16)
    ks[0] = jnp.where(head0, k, jnp.where(lane == HD, mb, 0.0)).astype(BF16)
    ks[1] = jnp.where(head0, jnp.where(lane == 0, mb, 0.0), k).astype(BF16)

    def block(j, carry):
        rows = pl.ds(pl.multiple_of(j * QB, QB), QB)
        outs, stats = [], []
        for head in range(2):
            s = lax.dot_general(qs[head, rows, :], ks[head], NT, preferred_element_type=F32)
            m = jnp.max(s, axis=-1, keepdims=True)
            e = jnp.exp(s - m)
            total = jnp.sum(e, axis=-1, keepdims=True)
            p = (e * (1.0 / total)).astype(BF16)
            outs.append(jnp.dot(p, v_ref[...], preferred_element_type=F32))
            stats.append(m + jnp.log(total))
        o_ref[rows, :] = jnp.where(head0, outs[0], outs[1]).astype(BF16)
        st[rows, :] = jnp.where(head0, stats[0], stats[1])
        return carry

    lax.fori_loop(0, seq // QB, block, 0)
    st_t = st[...].T
    lse_ref[0] = jnp.concatenate([st_t[0:1]] * 4 + [st_t[HD:65]] * 4, axis=0)


def whole(*shape):
    return pl.BlockSpec(shape, lambda *i: (0,) * len(shape))


def head_blocks(parts, dim, first=0):
    return pl.BlockSpec((parts, HD, dim), lambda i: (0, i + first, 0))


def compiler_params():
    return pltpu.CompilerParams(dimension_semantics=("arbitrary",), vmem_limit_bytes=VMEM_LIMIT)


def cost(flops):
    return pl.CostEstimate(flops=flops, bytes_accessed=20_000_000, transcendentals=0)


def attn_fwd(h1, w0, w1, bias, cos_tab, sin_tab, mask_col):
    seq, dim = h1.shape
    heads = w0.shape[1] // HD
    pair = pl.BlockSpec((seq, LANES), lambda i: (0, i))
    head_w = head_blocks(3, dim)
    tab = whole(seq, LANES)
    act = jax.ShapeDtypeStruct((seq, heads * LANES), BF16)
    both = pltpu.VMEM((2, seq, LANES), BF16)
    return pl.pallas_call(
        attn_fwd_kernel,
        grid=(heads,),
        in_specs=[whole(seq, dim), head_w, head_w, pl.BlockSpec((1, 3, LANES), lambda i: (i, 0, 0)), tab, tab, tab],
        out_specs=[pair, pair, pair, pair, pl.BlockSpec((1, 8, seq), lambda i: (i, 0, 0))],
        out_shape=[act, act, act, act, jax.ShapeDtypeStruct((heads, 8, seq), F32)],
        scratch_shapes=[both, both, pltpu.VMEM((seq, LANES), F32)],
        compiler_params=compiler_params(),
        cost_estimate=cost(heads * seq * (dim + seq) * 1024),
        name="attn_fwd",
    )(h1, w0, w1, bias, cos_tab, sin_tab, mask_col)


def attn_bwd_kernel(h_ref, dx_ref, w0_ref, w1_ref, wo0_ref, wo1_ref, q_ref, k_ref, v_ref, o_ref, lse_ref, cos_ref, sin_ref, mb_ref,
                    dh_ref, gw0_ref, gw1_ref, gb_ref, qs, qz, ks, dos, kt, dqt, dk_acc, dv_acc):
    seq, _ = h_ref.shape
    lane = lax.broadcasted_iota(jnp.int32, (1, LANES), 1)
    first_half = (lane % HD) < 32
    head0 = lane < HD
    dx = dx_ref[...]
    wo = jnp.concatenate([wo0_ref[0], wo1_ref[0]], axis=0)
    d_o = lax.dot_general(dx, wo, NT, preferred_element_type=F32)
    dos[0] = jnp.where(head0, d_o, 0.0).astype(BF16)
    dos[1] = jnp.where(head0, 0.0, d_o).astype(BF16)
    gwo = jnp.dot(o_ref[...].T, dx, preferred_element_type=F32)
    gw0_ref[3] = gwo[:HD]
    gw1_ref[3] = gwo[HD:]
    q, k, mb = q_ref[...].astype(F32), k_ref[...].astype(F32), mb_ref[...]
    qs[0] = jnp.where(head0, q, jnp.where(lane == HD, 1.0, 0.0)).astype(BF16)
    qs[1] = jnp.where(head0, jnp.where(lane == 0, 1.0, 0.0), q).astype(BF16)
    qz[0] = jnp.where(head0, q, 0.0).astype(BF16)
    qz[1] = jnp.where(head0, 0.0, q).astype(BF16)
    ks[0] = jnp.where(head0, k, jnp.where(lane == HD, mb, 0.0)).astype(BF16)
    ks[1] = jnp.where(head0, jnp.where(lane == 0, mb, 0.0), k).astype(BF16)
    kt[...] = k_ref[...].T
    dk_acc[...] = jnp.zeros_like(dk_acc)
    dv_acc[...] = jnp.zeros_like(dv_acc)

    def block(j, carry):
        rows = pl.ds(pl.multiple_of(j * QB, QB), QB)
        for head in range(2):
            s_t = lax.dot_general(ks[head], qs[head, rows, :], NT, preferred_element_type=F32)
            p_t = jnp.exp(s_t - lse_ref[0, 4 * head:4 * head + 1, rows])
            do_b = dos[head, rows, :]
            dp_t = lax.dot_general(v_ref[...], do_b, NT, preferred_element_type=F32)
            corr = jnp.sum(p_t * dp_t, axis=0, keepdims=True)
            ds_t = (p_t * (dp_t - corr)).astype(BF16)
            dv_acc[...] += jnp.dot(p_t.astype(BF16), do_b, preferred_element_type=F32)
            dk_acc[...] += jnp.dot(ds_t, qz[head, rows, :], preferred_element_type=F32)
            dqt[HD * head:HD * head + HD, rows] = jnp.dot(kt[HD * head:HD * head + HD, :], ds_t, preferred_element_type=F32)
        return carry

    lax.fori_loop(0, seq // QB, block, 0)
    cos, sin = cos_ref[...], sin_ref[...]
    dq, dk, dv = dqt[...].T, dk_acc[...], dv_acc[...]
    dq = (dq * cos - swap_halves(dq, first_half) * sin) * 0.125
    dk = dk * cos - swap_halves(dk, first_half) * sin
    d_all = jnp.concatenate([dq, dk, dv], axis=1)
    sums = jnp.sum(d_all, axis=0, keepdims=True)
    gb_ref[0] = jnp.concatenate([sums[:, :LANES], sums[:, LANES:256], sums[:, 256:], jnp.zeros((5, LANES), F32)], axis=0)
    d_low = d_all.astype(BF16)
    w = pair_rows(w0_ref, w1_ref)
    part = jnp.dot(d_low, w, preferred_element_type=F32)
    gw = jnp.dot(d_low.T, h_ref[...], preferred_element_type=F32)
    for i in range(3):
        gw0_ref[i] = gw[LANES * i:LANES * i + HD]
        gw1_ref[i] = gw[LANES * i + HD:LANES * i + LANES]

    @pl.when(pl.program_id(0) == 0)
    def _():
        dh_ref[...] = part

    @pl.when(pl.program_id(0) > 0)
    def _():
        dh_ref[...] += part


def attn_bwd(h1, d_x1, w0, w1, wo0, wo1, q, k, v, o, lse, cos_tab, sin_tab, mask_col, first, count):
    seq, dim = h1.shape
    pair = pl.BlockSpec((seq, LANES), lambda i: (0, i + first))
    head_w = head_blocks(3, dim, first)
    head_o = pl.BlockSpec((1, HD, dim), lambda i: (i + first, 0, 0))
    tab = whole(seq, LANES)
    gw = jax.ShapeDtypeStruct((4, count * HD, dim), F32)
    half = pltpu.VMEM((2, seq, LANES), BF16)
    acc = pltpu.VMEM((seq, LANES), F32)
    return pl.pallas_call(
        attn_bwd_kernel,
        grid=(count,),
        in_specs=[whole(seq, dim), whole(seq, dim), head_w, head_w, head_o, head_o, pair, pair, pair, pair,
                  pl.BlockSpec((1, 8, seq), lambda i: (i + first, 0, 0)), tab, tab, tab],
        out_specs=[whole(seq, dim), head_blocks(4, dim), head_blocks(4, dim), pl.BlockSpec((1, 8, LANES), lambda i: (i, 0, 0))],
        out_shape=[jax.ShapeDtypeStruct((seq, dim), F32), gw, gw, jax.ShapeDtypeStruct((count, 8, LANES), F32)],
        scratch_shapes=[half, half, half, half, pltpu.VMEM((LANES, seq), BF16), pltpu.VMEM((LANES, seq), F32), acc, acc],
        compiler_params=compiler_params(),
        cost_estimate=cost(count * seq * (dim + seq) * 2048),
        name="attn_bwd",
    )(h1, d_x1, w0, w1, wo0, wo1, q, k, v, o, lse, cos_tab, sin_tab, mask_col)


def gelu_terms(pre):
    erf_term = lax.erf(pre * INV_SQRT2)
    act = 0.5 * pre * (1.0 + erf_term)
    slope = 0.5 * (1.0 + erf_term) + pre * jnp.exp(-0.5 * pre * pre) * INV_SQRT_2PI
    return act, slope


def mlp_kernel(tiles, n_w, chained, emit, *refs):
    refs = list(refs)
    take = lambda n: [refs.pop(0) for _ in range(n)]
    h_ref, dy_ref, b_ref = take(3)
    ups, downs = take(n_w), take(n_w)
    before = take(2) if chained else None
    y_ref, dh_ref = take(2)
    act_ref, dpre_ref, sum_ref = take(3) if emit else (None,) * 3
    wu, wd, sem = refs
    width = wu.shape[2]
    step = pl.program_id(0)
    copies = []
    for t, (src, part) in enumerate(tiles):
        cols = pl.ds(part * width, width)
        copies.append((pltpu.make_async_copy(ups[src].at[:, cols], wu.at[t], sem.at[0, t]),
                       pltpu.make_async_copy(downs[src].at[cols, :], wd.at[t], sem.at[1, t])))

    @pl.when(step == 0)
    def _():
        for up, down in copies:
            up.start()
            down.start()

    y_sum, dh_sum = (before[0][...], before[1][...]) if chained else (None, None)
    for t in range(len(tiles)):
        @pl.when(step == 0)
        def _(t=t):
            copies[t][0].wait()
            copies[t][1].wait()

        pre = jnp.dot(h_ref[...], wu[t], preferred_element_type=F32) + b_ref[t]
        act, slope = gelu_terms(pre)
        act = act.astype(BF16)
        d_act = lax.dot_general(dy_ref[...], wd[t], NT, preferred_element_type=F32)
        y_part = jnp.dot(act, wd[t], preferred_element_type=F32)
        d_pre = d_act * slope
        d_low = d_pre.astype(BF16)
        dh_part = lax.dot_general(d_low, wu[t], NT, preferred_element_type=F32)
        y_sum = y_part if y_sum is None else y_sum + y_part
        dh_sum = dh_part if dh_sum is None else dh_sum + dh_part
        if emit:
            cols = slice(t * width, (t + 1) * width)
            act_ref[:, cols] = act
            dpre_ref[:, cols] = d_low
            total = jnp.broadcast_to(jnp.sum(d_pre, axis=0, keepdims=True), (8, width))
            sum_ref[:, cols] = total + jnp.where(step == 0, 0.0, sum_ref[:, cols])
    y_ref[...] = y_sum
    dh_ref[...] = dh_sum


def mlp_chain(h2, d_y, bias, ups, downs, before=(), emit=False):
    seq, dim = h2.shape
    width = bias.shape[2]
    tiles = [(i, p) for i, w in enumerate(ups) for p in range(w.shape[1] // width)]
    rows = pl.BlockSpec((QB, dim), lambda j: (j, 0))
    wide = pl.BlockSpec((QB, len(tiles) * width), lambda j: (j, 0))
    hbm = pl.BlockSpec(memory_space=pl.ANY)
    out = jax.ShapeDtypeStruct((seq, dim), F32)
    low = jax.ShapeDtypeStruct((seq, len(tiles) * width), BF16)
    out_specs, out_shape = [rows, rows], [out, out]
    if emit:
        out_specs += [wide, wide, whole(8, len(tiles) * width)]
        out_shape += [low, low, jax.ShapeDtypeStruct((8, len(tiles) * width), F32)]
    return pl.pallas_call(
        functools.partial(mlp_kernel, tiles, len(ups), bool(before), emit),
        grid=(seq // QB,),
        in_specs=[rows, rows, whole(*bias.shape)] + [hbm] * (2 * len(ups)) + [rows] * len(before),
        out_specs=out_specs,
        out_shape=out_shape,
        scratch_shapes=[pltpu.VMEM((len(tiles), dim, width), BF16), pltpu.VMEM((len(tiles), width, dim), BF16),
                        pltpu.SemaphoreType.DMA((2, len(tiles)))],
        compiler_params=compiler_params(),
        cost_estimate=cost(len(tiles) * 8 * seq * dim * width),
        name="mlp_chain",
    )(h2, d_y, bias, *ups, *downs, *before)


def join_kernel(places, n_src, idx_ref, *refs):
    srcs, outs, sem = refs[:n_src], refs[n_src:-1], refs[-1]
    rows = srcs[0].shape[1]
    copies = []
    for p, (src, out, slot) in enumerate(places):
        copies.append(pltpu.make_async_copy(srcs[src].at[idx_ref[p]], outs[out].at[pl.ds(slot * rows, rows)], sem.at[p]))
    for c in copies:
        c.start()
    for c in copies:
        c.wait()


def join(pieces):
    arrays, places, index = [], [], []
    for out, row in enumerate(pieces):
        for slot, (array, i) in enumerate(row):
            at = [k for k, a in enumerate(arrays) if a is array]
            if not at:
                arrays.append(array)
            places.append((at[0] if at else len(arrays) - 1, out, slot))
            index.append(i)
    _, rows, dim = arrays[0].shape
    out = jax.ShapeDtypeStruct((len(pieces[0]) * rows, dim), arrays[0].dtype)
    vmem = pl.BlockSpec(memory_space=pltpu.VMEM)
    return pl.pallas_call(
        functools.partial(join_kernel, places, len(arrays)),
        in_specs=[pl.BlockSpec(memory_space=pltpu.SMEM)] + [pl.BlockSpec(memory_space=pl.ANY)] * len(arrays),
        out_specs=[vmem] * len(pieces),
        out_shape=[out] * len(pieces),
        scratch_shapes=[pltpu.SemaphoreType.DMA((len(places),))],
        cost_estimate=cost(10_000_000),
        name="join_rows",
    )(jnp.stack(index).astype(jnp.int32), *arrays)


def add_kernel(split, a_ref, b_ref, c0_ref, c1_ref, q_ref, o_ref):
    part, head = pl.program_id(0), pl.program_id(1)
    total = (a_ref[0] + b_ref[0]) + jnp.where(head < split, c0_ref[0], c1_ref[0])

    @pl.when(part < 3)
    def _():
        q_ref[0] = total

    @pl.when(part == 3)
    def _():
        o_ref[...] = total


def add_grads(a, b, c0, c1):
    parts, size, dim = a.shape
    heads, split = size // HD, c0.shape[1] // HD
    block = lambda f: pl.BlockSpec((1, HD, dim), f)
    last = parts - 1
    return pl.pallas_call(
        functools.partial(add_kernel, split),
        grid=(parts, heads),
        in_specs=[block(lambda p, i: (p, i, 0)), block(lambda p, i: (p, i, 0)),
                  block(lambda p, i: (p, jnp.minimum(i, split - 1), 0)), block(lambda p, i: (p, jnp.maximum(i - split, 0), 0))],
        out_specs=[block(lambda p, i: (jnp.minimum(p, last - 1), jnp.where(p < last, i, heads - 1), 0)),
                   pl.BlockSpec((HD, dim), lambda p, i: (jnp.where(p < last, 0, i), 0))],
        out_shape=[jax.ShapeDtypeStruct((last, size, dim), F32), jax.ShapeDtypeStruct((size, dim), F32)],
        cost_estimate=cost(10_000_000),
        name="add_grads",
    )(a, b, c0, c1)


def xor_move(value, bits):
    return lax.ppermute(value, 'tp', [(i, i ^ bits) for i in range(4)])


def swap_groups(value):
    return lax.ppermute(value, 'dp', [(0, 1), (1, 0)])


def after(value, *others):
    return lax.optimization_barrier((value,) + others)[0]


def solution(mesh):
    act_spec = P('dp', 'tp', None)
    rep_vec = P(None)
    part_vec = P('dp')
    in_specs = (act_spec, act_spec, P('dp', None), rep_vec, rep_vec, P(None, None, 'tp', None), P(None, 'tp', None),
                P('tp', None, None), rep_vec, rep_vec, rep_vec, P(None, 'tp'), P('tp'), P('tp', None), rep_vec)
    out_specs = (act_spec, act_spec, part_vec, part_vec, P('dp', None, 'tp', None), P('dp', 'tp', None),
                 P(('dp', 'tp'), None, None), part_vec, part_vec, part_vec, P('dp', 'tp'), P(('dp', 'tp')),
                 P(('dp', 'tp'), None), part_vec)

    def layer(x_in, grad_y, pad_mask, ln1_gain, ln1_bias, w_qkv, b_qkv, w_out, b_out, ln2_gain, ln2_bias, w_up, b_up, w_down, b_down):
        me = lax.axis_index('tp')
        group = lax.axis_index('dp')
        core, chip = me % 2, me // 2
        _, rows, dim = x_in.shape
        heads = w_out.shape[0]
        cols = w_up.shape[1]
        half = cols // 2

        def pick(blocks, index):
            return lax.dynamic_index_in_dim(blocks, index, 0, keepdims=False)

        def to_blocks(value):
            v = [value[s * rows:(s + 1) * rows] for s in range(4)]
            v = [v[0]] + [xor_move(v[s], s) for s in (1, 2, 3)]
            low = [jnp.where(core == 1, a, b) for a, b in ((v[1], v[0]), (v[0], v[1]))]
            high = [jnp.where(core == 1, a, b) for a, b in ((v[3], v[2]), (v[2], v[3]))]
            first = [jnp.where(chip == 1, b, a) for a, b in zip(low, high)]
            last = [jnp.where(chip == 1, a, b) for a, b in zip(low, high)]
            return jnp.stack(first + last)

        x_slots = [pick(x_in, me ^ s) for s in range(4)]
        x_seq = jnp.concatenate([x_slots[0]] + [xor_move(x_slots[s], s) for s in (1, 2, 3)])
        small = jnp.concatenate([b_up, jnp.transpose(b_qkv, (1, 0, 2)).reshape(-1)])
        smalls = [small] + [xor_move(small, s) for s in (1, 2, 3)]
        b_ups = [v[:cols].reshape(2, 1, half) for v in smalls]
        b_qkvs = [v[cols:].reshape(heads, 3, HD) for v in smalls]
        w_heads = jnp.transpose(w_qkv, (0, 2, 3, 1)).reshape(3, heads * HD, dim)
        wq = [w_heads, xor_move(w_heads, 1), xor_move(w_heads, 2)]
        wo = [w_out, xor_move(w_out, 1), xor_move(w_out, 2)]
        dya2 = xor_move(lax.dynamic_slice_in_dim(grad_y, (1 - chip) * 2, 2, 0), 2)
        dy1 = xor_move(grad_y, 1)
        up2 = xor_move(lax.dynamic_slice_in_dim(w_up, group * half, half, 1), 2)
        down2 = xor_move(lax.dynamic_slice_in_dim(w_down, group * half, half, 0), 2)
        ups = [w_up, xor_move(w_up, 1)]
        downs = [w_down, xor_move(w_down, 1)]

        positions = jnp.concatenate([(me ^ s) * rows + jnp.arange(rows) for s in range(4)])
        cos_tab, sin_tab = rope_tables(positions, HD)
        length = jnp.sum((pick(pad_mask, me) > 0).astype(jnp.int32))
        mask_col = jnp.broadcast_to(jnp.where(positions < length, 0.0, NEG_LARGE).astype(F32)[:, None], (4 * rows, LANES))
        x_f = x_seq.astype(F32)
        h1_f, x_hat1, inv_std1 = layer_norm(x_f, ln1_gain, ln1_bias)
        h1 = h1_f.astype(BF16)

        def pair_bias(a, b):
            return jnp.concatenate([a, b], axis=-1)

        fwd_a = attn_fwd(h1, wq[0], wq[1], pair_bias(b_qkvs[0], b_qkvs[1]), cos_tab, sin_tab, mask_col)
        wq.append(xor_move(wq[2], 1))
        fwd_b = attn_fwd(h1, wq[2], wq[3], pair_bias(b_qkvs[2], b_qkvs[3]), cos_tab, sin_tab, mask_col)
        wo.append(xor_move(wo[2], 1))

        def pair_out(a, b):
            return jnp.stack([a, b], axis=1).reshape(2 * heads * HD, dim)

        attn_sum = jnp.dot(fwd_a[3], pair_out(wo[0], wo[1]), preferred_element_type=F32)
        attn_sum = attn_sum + jnp.dot(fwd_b[3], pair_out(wo[2], wo[3]), preferred_element_type=F32)
        x1_f = (x_f + (attn_sum + b_out)).astype(BF16).astype(F32)
        h2_f, x_hat2, inv_std2 = layer_norm(x1_f, ln2_gain, ln2_bias)
        h2 = h2_f.astype(BF16)
        dya3 = xor_move(dya2, 1)
        h2_next = xor_move(h2, 1)
        nxt, oth = me ^ 1, 1 - core
        d_y, d_y_next = join([[(grad_y, me), (dy1, me), (dya2, core), (dya3, core)],
                              [(dy1, nxt), (grad_y, nxt), (dya3, oth), (dya2, oth)]])
        dy_f = d_y.astype(F32)

        def grad_dot(a, b):
            return lax.dot_general(a, b, (((0,), (0,)), ((), ())), preferred_element_type=F32)

        y_a, dh2_a, act0, dpre0, sum0 = mlp_chain(h2, d_y, b_ups[0], ups[:1], downs[:1], emit=True)
        up_y = swap_groups(after(up2, y_a))
        y_a, dh2_a, act1, dpre1, sum1 = mlp_chain(h2, d_y, b_ups[1], ups[1:], downs[1:], before=(y_a, dh2_a), emit=True)
        act_next, dpre_next, sum_next = (xor_move(v, 1) for v in (act1, dpre1, sum1))
        h2_far = xor_move(after(h2, down2), 2)
        dyb2 = xor_move(after(lax.dynamic_slice_in_dim(grad_y, chip * 2, 2, 0), down2), 2)
        own_up, own_down = grad_dot(after(h2, y_a), dpre0), grad_dot(act0, after(d_y, y_a))
        down_y = swap_groups(after(down2, y_a))
        up3, down3 = xor_move(after(up2, y_a), 1), xor_move(after(down2, y_a), 1)
        far_bias = [jnp.where(group == 0, v, v[::-1]) for v in b_ups[2:]]
        y_c, dh2_c = mlp_chain(after(h2, own_up, own_down), d_y, jnp.concatenate([v[:1] for v in far_bias]), [up2, up3], [down2, down3],
                               before=(y_a, dh2_a))
        up3_y, down3_y = xor_move(after(up_y, own_up), 1), xor_move(after(down_y, y_c), 1)
        near_up = own_up + grad_dot(after(h2_next, y_c), dpre_next)
        near_down = own_down + grad_dot(act_next, after(d_y_next, y_c))
        y_d, d_h2 = mlp_chain(after(h2, near_up, near_down), d_y, jnp.concatenate([v[1:] for v in far_bias]), [up_y, up3_y], [down_y, down3_y],
                              before=(y_c, dh2_c))
        y_seq = (x1_f + (y_d + b_down)).astype(BF16)
        y_out = to_blocks(y_seq)
        d_x1 = dy_f + layer_norm_grad(d_h2, x_hat2, inv_std2, ln2_gain)
        d_x1_b = d_x1.astype(BF16)

        def backward(i, fwd, d_mid, first, count):
            q, k, v, o, lse = fwd
            return attn_bwd(h1, d_mid, wq[i], wq[i + 1], wo[i], wo[i + 1], q, k, v, o, lse, cos_tab, sin_tab, mask_col, first, count)

        split = 3
        bwd_b = backward(2, fwd_b, d_x1_b, 0, split)
        g_far = bwd_b[1] + xor_move(bwd_b[2], 1)
        g_across = xor_move(g_far, 2)
        bwd_c = backward(2, fwd_b, after(d_x1_b, g_far), split, heads - split)
        g_far_c = bwd_c[1] + xor_move(bwd_c[2], 1)
        g_across_c = xor_move(g_far_c, 2)
        dyb3 = xor_move(after(dyb2, bwd_b[0]), 1)
        h2_far_next = xor_move(after(h2_far, bwd_b[0]), 1)
        bwd_a = backward(0, fwd_a, after(d_x1_b, g_far_c), 0, heads)
        d_h1 = (bwd_b[0] + bwd_c[0]) + bwd_a[0]
        grad_x_seq = (d_x1 + layer_norm_grad(d_h1, x_hat1, inv_std1, ln1_gain)).astype(BF16)
        sums = jnp.concatenate([jnp.sum(v, axis=0) for v in (dy_f, d_h2 * x_hat2, d_h2, d_x1, d_h1 * x_hat1, d_h1)])
        gb = []
        for part in (bwd_a[3], jnp.concatenate([bwd_b[3], bwd_c[3]])):
            part = jnp.transpose(part[:, :3], (1, 0, 2))
            gb += [part[..., :HD].reshape(-1), part[..., HD:].reshape(-1)]
        packs = [jnp.concatenate([sums, v]) for v in gb]
        packs = [packs[0]] + [xor_move(packs[s], s) for s in (1, 2, 3)]
        totals = (packs[0] + packs[1]) + (packs[2] + packs[3])
        sums, grad_b_qkv = totals[:6 * dim].reshape(6, dim), totals[6 * dim:].reshape(3, heads, HD)
        grad_x = to_blocks(grad_x_seq)

        far, diag = me ^ 2, me ^ 3
        dy_far = join([[(dyb2, core), (dyb3, core), (grad_y, far), (dy1, far), (dyb3, oth), (dyb2, oth), (dy1, diag), (grad_y, diag)]])[0]
        h2_other = jnp.concatenate([after(h2_far, grad_x_seq), h2_far_next])
        pre_act = jnp.dot(h2_other, w_up, preferred_element_type=F32) + b_up
        act, gelu_slope = gelu_terms(pre_act)
        grad_w_down = near_down + grad_dot(act.astype(BF16), dy_far)
        d_pre = lax.dot_general(dy_far, w_down, NT, preferred_element_type=F32) * gelu_slope
        grad_w_up = near_up + grad_dot(h2_other, d_pre.astype(BF16))
        grad_b_up = (sum0[0] + sum_next[0]) + jnp.sum(d_pre, axis=0)
        grads_q, grad_w_out = add_grads(bwd_a[1], xor_move(bwd_a[2], 1), g_across, g_across_c)
        grad_w_qkv = jnp.transpose(grads_q.reshape(3, heads, HD, dim), (0, 3, 1, 2))
        grad_w_out = grad_w_out.reshape(heads, HD, dim)
        return (y_out, grad_x, sums[4], sums[5], grad_w_qkv, grad_b_qkv, grad_w_out, sums[3],
                sums[1], sums[2], grad_w_up, grad_b_up, grad_w_down, sums[0])

    return jax.shard_map(layer, mesh=mesh, in_specs=in_specs, out_specs=out_specs, check_vma=False)
```

```python
import functools

import jax
import jax.numpy as jnp
from jax import lax
from jax.experimental import pallas as pl
from jax.experimental.pallas import tpu as pltpu
from jax.sharding import PartitionSpec as P


LN_EPS = 1e-5
ROPE_BASE = 10000.0
INV_SQRT2 = 0.7071067811865476
INV_SQRT_2PI = 0.3989422804014327
NEG_LARGE = -1e30
F32 = jnp.float32
BF16 = jnp.bfloat16
NT = (((1,), (1,)), ((), ()))
VMEM_LIMIT = 60 << 20
LANES = 128
HD = 64
QB = 256


def layer_norm(values, ln_gain, ln_bias):
    centered = values - jnp.mean(values, axis=-1, keepdims=True)
    inv_std = lax.rsqrt(jnp.mean(centered * centered, axis=-1, keepdims=True) + LN_EPS)
    x_hat = centered * inv_std
    return x_hat * ln_gain + ln_bias, x_hat, inv_std


def layer_norm_grad(d_out, x_hat, inv_std, ln_gain):
    d_hat = d_out * ln_gain
    return inv_std * (d_hat - jnp.mean(d_hat, axis=-1, keepdims=True) - x_hat * jnp.mean(d_hat * x_hat, axis=-1, keepdims=True))


def rope_tables(positions, head_dim):
    half_dim = head_dim // 2
    inv_freq = ROPE_BASE ** (-2.0 * jnp.arange(half_dim, dtype=F32) / head_dim)
    angles = positions.astype(F32)[:, None] * inv_freq[None, :]
    cos_half, sin_half = jnp.cos(angles), jnp.sin(angles)
    cos_tab = jnp.concatenate([cos_half] * 4, axis=-1)
    sin_tab = jnp.concatenate([-sin_half, sin_half, -sin_half, sin_half], axis=-1)
    return cos_tab, sin_tab


def swap_halves(t, first_half):
    return jnp.where(first_half, pltpu.roll(t, 96, 1), pltpu.roll(t, 32, 1))


def pair_rows(ref0, ref1):
    return jnp.concatenate([r[i] for i in range(3) for r in (ref0, ref1)], axis=0)


def attn_fwd_kernel(h_ref, w0_ref, w1_ref, b_ref, cos_ref, sin_ref, mb_ref, q_ref, k_ref, v_ref, o_ref, lse_ref, qs, ks, st):
    seq = h_ref.shape[0]
    lane = lax.broadcasted_iota(jnp.int32, (1, LANES), 1)
    first_half = (lane % HD) < 32
    head0 = lane < HD
    w = pair_rows(w0_ref, w1_ref)
    t = lax.dot_general(h_ref[...], w, NT, preferred_element_type=F32)
    cos, sin = cos_ref[...], sin_ref[...]
    tq = (t[:, :LANES] + b_ref[0, 0:1]) * 0.125
    tk = t[:, LANES:256] + b_ref[0, 1:2]
    q = (tq * cos + swap_halves(tq, first_half) * sin).astype(BF16)
    k = (tk * cos + swap_halves(tk, first_half) * sin).astype(BF16)
    v_ref[...] = (t[:, 256:] + b_ref[0, 2:3]).astype(BF16)
    q_ref[...] = q
    k_ref[...] = k
    q, k = q.astype(F32), k.astype(F32)
    mb = mb_ref[...]
    qs[0] = jnp.where(head0, q, jnp.where(lane == HD, 1.0, 0.0)).astype(BF16)
    qs[1] = jnp.where(head0, jnp.where(lane == 0, 1.0, 0.0), q).astype(BF16)
    ks[0] = jnp.where(head0, k, jnp.where(lane == HD, mb, 0.0)).astype(BF16)
    ks[1] = jnp.where(head0, jnp.where(lane == 0, mb, 0.0), k).astype(BF16)

    def block(j, carry):
        rows = pl.ds(pl.multiple_of(j * QB, QB), QB)
        outs, stats = [], []
        for head in range(2):
            s = lax.dot_general(qs[head, rows, :], ks[head], NT, preferred_element_type=F32)
            m = jnp.max(s, axis=-1, keepdims=True)
            e = jnp.exp(s - m)
            total = jnp.sum(e, axis=-1, keepdims=True)
            p = (e * (1.0 / total)).astype(BF16)
            outs.append(jnp.dot(p, v_ref[...], preferred_element_type=F32))
            stats.append(m + jnp.log(total))
        o_ref[rows, :] = jnp.where(head0, outs[0], outs[1]).astype(BF16)
        st[rows, :] = jnp.where(head0, stats[0], stats[1])
        return carry

    lax.fori_loop(0, seq // QB, block, 0)
    st_t = st[...].T
    lse_ref[0] = jnp.concatenate([st_t[0:1]] * 4 + [st_t[HD:65]] * 4, axis=0)


def whole(*shape):
    return pl.BlockSpec(shape, lambda *i: (0,) * len(shape))


def head_blocks(parts, dim, first=0):
    return pl.BlockSpec((parts, HD, dim), lambda i: (0, i + first, 0))


def compiler_params():
    return pltpu.CompilerParams(dimension_semantics=("arbitrary",), vmem_limit_bytes=VMEM_LIMIT)


def cost(flops):
    return pl.CostEstimate(flops=flops, bytes_accessed=20_000_000, transcendentals=0)


def attn_fwd(h1, w0, w1, bias, cos_tab, sin_tab, mask_col):
    seq, dim = h1.shape
    heads = w0.shape[1] // HD
    pair = pl.BlockSpec((seq, LANES), lambda i: (0, i))
    head_w = head_blocks(3, dim)
    tab = whole(seq, LANES)
    act = jax.ShapeDtypeStruct((seq, heads * LANES), BF16)
    both = pltpu.VMEM((2, seq, LANES), BF16)
    return pl.pallas_call(
        attn_fwd_kernel,
        grid=(heads,),
        in_specs=[whole(seq, dim), head_w, head_w, pl.BlockSpec((1, 3, LANES), lambda i: (i, 0, 0)), tab, tab, tab],
        out_specs=[pair, pair, pair, pair, pl.BlockSpec((1, 8, seq), lambda i: (i, 0, 0))],
        out_shape=[act, act, act, act, jax.ShapeDtypeStruct((heads, 8, seq), F32)],
        scratch_shapes=[both, both, pltpu.VMEM((seq, LANES), F32)],
        compiler_params=compiler_params(),
        cost_estimate=cost(heads * seq * (dim + seq) * 1024),
        name="attn_fwd",
    )(h1, w0, w1, bias, cos_tab, sin_tab, mask_col)


def attn_bwd_kernel(h_ref, dx_ref, w0_ref, w1_ref, wo0_ref, wo1_ref, q_ref, k_ref, v_ref, o_ref, lse_ref, cos_ref, sin_ref, mb_ref,
                    dh_ref, gw0_ref, gw1_ref, gb_ref, qs, qz, ks, dos, kt, dqt, dk_acc, dv_acc):
    seq, _ = h_ref.shape
    lane = lax.broadcasted_iota(jnp.int32, (1, LANES), 1)
    first_half = (lane % HD) < 32
    head0 = lane < HD
    dx = dx_ref[...]
    wo = jnp.concatenate([wo0_ref[0], wo1_ref[0]], axis=0)
    d_o = lax.dot_general(dx, wo, NT, preferred_element_type=F32)
    dos[0] = jnp.where(head0, d_o, 0.0).astype(BF16)
    dos[1] = jnp.where(head0, 0.0, d_o).astype(BF16)
    gwo = jnp.dot(o_ref[...].T, dx, preferred_element_type=F32)
    gw0_ref[3] = gwo[:HD]
    gw1_ref[3] = gwo[HD:]
    q, k, mb = q_ref[...].astype(F32), k_ref[...].astype(F32), mb_ref[...]
    qs[0] = jnp.where(head0, q, jnp.where(lane == HD, 1.0, 0.0)).astype(BF16)
    qs[1] = jnp.where(head0, jnp.where(lane == 0, 1.0, 0.0), q).astype(BF16)
    qz[0] = jnp.where(head0, q, 0.0).astype(BF16)
    qz[1] = jnp.where(head0, 0.0, q).astype(BF16)
    ks[0] = jnp.where(head0, k, jnp.where(lane == HD, mb, 0.0)).astype(BF16)
    ks[1] = jnp.where(head0, jnp.where(lane == 0, mb, 0.0), k).astype(BF16)
    kt[...] = k_ref[...].T
    dk_acc[...] = jnp.zeros_like(dk_acc)
    dv_acc[...] = jnp.zeros_like(dv_acc)

    def block(j, carry):
        rows = pl.ds(pl.multiple_of(j * QB, QB), QB)
        for head in range(2):
            s_t = lax.dot_general(ks[head], qs[head, rows, :], NT, preferred_element_type=F32)
            p_t = jnp.exp(s_t - lse_ref[0, 4 * head:4 * head + 1, rows])
            do_b = dos[head, rows, :]
            dp_t = lax.dot_general(v_ref[...], do_b, NT, preferred_element_type=F32)
            corr = jnp.sum(p_t * dp_t, axis=0, keepdims=True)
            ds_t = (p_t * (dp_t - corr)).astype(BF16)
            dv_acc[...] += jnp.dot(p_t.astype(BF16), do_b, preferred_element_type=F32)
            dk_acc[...] += jnp.dot(ds_t, qz[head, rows, :], preferred_element_type=F32)
            dqt[HD * head:HD * head + HD, rows] = jnp.dot(kt[HD * head:HD * head + HD, :], ds_t, preferred_element_type=F32)
        return carry

    lax.fori_loop(0, seq // QB, block, 0)
    cos, sin = cos_ref[...], sin_ref[...]
    dq, dk, dv = dqt[...].T, dk_acc[...], dv_acc[...]
    dq = (dq * cos - swap_halves(dq, first_half) * sin) * 0.125
    dk = dk * cos - swap_halves(dk, first_half) * sin
    d_all = jnp.concatenate([dq, dk, dv], axis=1)
    sums = jnp.sum(d_all, axis=0, keepdims=True)
    gb_ref[0] = jnp.concatenate([sums[:, :LANES], sums[:, LANES:256], sums[:, 256:], jnp.zeros((5, LANES), F32)], axis=0)
    d_low = d_all.astype(BF16)
    w = pair_rows(w0_ref, w1_ref)
    part = jnp.dot(d_low, w, preferred_element_type=F32)
    gw = jnp.dot(d_low.T, h_ref[...], preferred_element_type=F32)
    for i in range(3):
        gw0_ref[i] = gw[LANES * i:LANES * i + HD]
        gw1_ref[i] = gw[LANES * i + HD:LANES * i + LANES]

    @pl.when(pl.program_id(0) == 0)
    def _():
        dh_ref[...] = part

    @pl.when(pl.program_id(0) > 0)
    def _():
        dh_ref[...] += part


def attn_bwd(h1, d_x1, w0, w1, wo0, wo1, q, k, v, o, lse, cos_tab, sin_tab, mask_col, first, count):
    seq, dim = h1.shape
    pair = pl.BlockSpec((seq, LANES), lambda i: (0, i + first))
    head_w = head_blocks(3, dim, first)
    head_o = pl.BlockSpec((1, HD, dim), lambda i: (i + first, 0, 0))
    tab = whole(seq, LANES)
    gw = jax.ShapeDtypeStruct((4, count * HD, dim), F32)
    half = pltpu.VMEM((2, seq, LANES), BF16)
    acc = pltpu.VMEM((seq, LANES), F32)
    return pl.pallas_call(
        attn_bwd_kernel,
        grid=(count,),
        in_specs=[whole(seq, dim), whole(seq, dim), head_w, head_w, head_o, head_o, pair, pair, pair, pair,
                  pl.BlockSpec((1, 8, seq), lambda i: (i + first, 0, 0)), tab, tab, tab],
        out_specs=[whole(seq, dim), head_blocks(4, dim), head_blocks(4, dim), pl.BlockSpec((1, 8, LANES), lambda i: (i, 0, 0))],
        out_shape=[jax.ShapeDtypeStruct((seq, dim), F32), gw, gw, jax.ShapeDtypeStruct((count, 8, LANES), F32)],
        scratch_shapes=[half, half, half, half, pltpu.VMEM((LANES, seq), BF16), pltpu.VMEM((LANES, seq), F32), acc, acc],
        compiler_params=compiler_params(),
        cost_estimate=cost(count * seq * (dim + seq) * 2048),
        name="attn_bwd",
    )(h1, d_x1, w0, w1, wo0, wo1, q, k, v, o, lse, cos_tab, sin_tab, mask_col)


def gelu_terms(pre):
    erf_term = lax.erf(pre * INV_SQRT2)
    act = 0.5 * pre * (1.0 + erf_term)
    slope = 0.5 * (1.0 + erf_term) + pre * jnp.exp(-0.5 * pre * pre) * INV_SQRT_2PI
    return act, slope


def mlp_kernel(n_w, chained, emit, *refs):
    refs = list(refs)
    take = lambda n: [refs.pop(0) for _ in range(n)]
    h_ref, dy_ref, b_ref = take(3)
    ups, downs = take(n_w), take(n_w)
    before = take(2) if chained else None
    y_ref, dh_ref = take(2)
    act_ref, dpre_ref, sum_ref = take(3) if emit else (None,) * 3
    wu, wd, sem = refs
    step = pl.program_id(0)
    width = wu.shape[0] // n_w
    copies = []
    for t in range(n_w):
        cols = pl.ds(t * width, width)
        copies.append((pltpu.make_async_copy(ups[t], wu.at[:, cols], sem.at[0, t]), pltpu.make_async_copy(downs[t], wd.at[cols, :], sem.at[1, t])))

    @pl.when(step == 0)
    def _():
        for up, down in copies:
            up.start()
            down.start()

    @pl.when(step == 0)
    def _():
        for up, down in copies:
            up.wait()
            down.wait()

    pre = jnp.dot(h_ref[...], wu[...], preferred_element_type=F32) + b_ref[...]
    act, slope = gelu_terms(pre)
    act = act.astype(BF16)
    d_pre = lax.dot_general(dy_ref[...], wd[...], NT, preferred_element_type=F32) * slope
    d_low = d_pre.astype(BF16)
    y_part = jnp.dot(act, wd[...], preferred_element_type=F32)
    dh_part = lax.dot_general(d_low, wu[...], NT, preferred_element_type=F32)
    y_ref[...] = before[0][...] + y_part if chained else y_part
    dh_ref[...] = before[1][...] + dh_part if chained else dh_part
    if emit:
        act_ref[...] = act
        dpre_ref[...] = d_low
        total = jnp.broadcast_to(jnp.sum(d_pre, axis=0, keepdims=True), sum_ref.shape)
        sum_ref[...] = total + jnp.where(step == 0, 0.0, sum_ref[...])


def mlp_chain(h2, d_y, bias, ups, downs, before=(), emit=False):
    seq, dim = h2.shape
    bias = bias.reshape(1, -1)
    width = bias.shape[1]
    rows = pl.BlockSpec((QB, dim), lambda j: (j, 0))
    wide = pl.BlockSpec((QB, width), lambda j: (j, 0))
    hbm = pl.BlockSpec(memory_space=pl.ANY)
    out = jax.ShapeDtypeStruct((seq, dim), F32)
    low = jax.ShapeDtypeStruct((seq, width), BF16)
    out_specs, out_shape = [rows, rows], [out, out]
    if emit:
        out_specs += [wide, wide, whole(8, width)]
        out_shape += [low, low, jax.ShapeDtypeStruct((8, width), F32)]
    return pl.pallas_call(
        functools.partial(mlp_kernel, len(ups), bool(before), emit),
        grid=(seq // QB,),
        in_specs=[rows, rows, whole(1, width)] + [hbm] * (2 * len(ups)) + [rows] * len(before),
        out_specs=out_specs,
        out_shape=out_shape,
        scratch_shapes=[pltpu.VMEM((dim, width), BF16), pltpu.VMEM((width, dim), BF16), pltpu.SemaphoreType.DMA((2, len(ups)))],
        compiler_params=compiler_params(),
        cost_estimate=cost(8 * seq * dim * width),
        name="mlp_chain",
    )(h2, d_y, bias, *ups, *downs, *before)


def join_kernel(places, n_src, idx_ref, *refs):
    srcs, outs, sem = refs[:n_src], refs[n_src:-1], refs[-1]
    rows = srcs[0].shape[1]
    copies = []
    for p, (src, out, slot) in enumerate(places):
        copies.append(pltpu.make_async_copy(srcs[src].at[idx_ref[p]], outs[out].at[pl.ds(slot * rows, rows)], sem.at[p]))
    for c in copies:
        c.start()
    for c in copies:
        c.wait()


def join(pieces):
    arrays, places, index = [], [], []
    for out, row in enumerate(pieces):
        for slot, (array, i) in enumerate(row):
            at = [k for k, a in enumerate(arrays) if a is array]
            if not at:
                arrays.append(array)
            places.append((at[0] if at else len(arrays) - 1, out, slot))
            index.append(i)
    _, rows, dim = arrays[0].shape
    out = jax.ShapeDtypeStruct((len(pieces[0]) * rows, dim), arrays[0].dtype)
    vmem = pl.BlockSpec(memory_space=pltpu.VMEM)
    return pl.pallas_call(
        functools.partial(join_kernel, places, len(arrays)),
        in_specs=[pl.BlockSpec(memory_space=pltpu.SMEM)] + [pl.BlockSpec(memory_space=pl.ANY)] * len(arrays),
        out_specs=[vmem] * len(pieces),
        out_shape=[out] * len(pieces),
        scratch_shapes=[pltpu.SemaphoreType.DMA((len(places),))],
        cost_estimate=cost(10_000_000),
        name="join_rows",
    )(jnp.stack(index).astype(jnp.int32), *arrays)


def add_kernel(split, a_ref, b_ref, c0_ref, c1_ref, q_ref, o_ref):
    part = pl.program_id(0)

    def store(dst):
        dst[:split] = (a_ref[0, :split] + b_ref[0, :split]) + c0_ref[0]
        dst[split:] = (a_ref[0, split:] + b_ref[0, split:]) + c1_ref[0]

    @pl.when(part < 3)
    def _():
        store(q_ref.at[0])

    @pl.when(part == 3)
    def _():
        store(o_ref)


def add_grads(a, b, c0, c1):
    parts, size, dim = a.shape
    last = parts - 1
    block = lambda v: pl.BlockSpec((1,) + v.shape[1:], lambda p: (p, 0, 0))
    return pl.pallas_call(
        functools.partial(add_kernel, c0.shape[1]),
        grid=(parts,),
        in_specs=[block(a), block(b), block(c0), block(c1)],
        out_specs=[pl.BlockSpec((1, size, dim), lambda p: (jnp.minimum(p, last - 1), 0, 0)), whole(size, dim)],
        out_shape=[jax.ShapeDtypeStruct((last, size, dim), F32), jax.ShapeDtypeStruct((size, dim), F32)],
        compiler_params=compiler_params(),
        cost_estimate=cost(10_000_000),
        name="add_grads",
    )(a, b, c0, c1)


def xor_move(value, bits):
    return lax.ppermute(value, 'tp', [(i, i ^ bits) for i in range(4)])


def swap_groups(value):
    return lax.ppermute(value, 'dp', [(0, 1), (1, 0)])


def after(value, *others):
    return lax.optimization_barrier((value,) + others)[0]


def solution(mesh):
    act_spec = P('dp', 'tp', None)
    rep_vec = P(None)
    part_vec = P('dp')
    in_specs = (act_spec, act_spec, P('dp', None), rep_vec, rep_vec, P(None, None, 'tp', None), P(None, 'tp', None),
                P('tp', None, None), rep_vec, rep_vec, rep_vec, P(None, 'tp'), P('tp'), P('tp', None), rep_vec)
    out_specs = (act_spec, act_spec, part_vec, part_vec, P('dp', None, 'tp', None), P('dp', 'tp', None),
                 P(('dp', 'tp'), None, None), part_vec, part_vec, part_vec, P('dp', 'tp'), P(('dp', 'tp')),
                 P(('dp', 'tp'), None), part_vec)

    def layer(x_in, grad_y, pad_mask, ln1_gain, ln1_bias, w_qkv, b_qkv, w_out, b_out, ln2_gain, ln2_bias, w_up, b_up, w_down, b_down):
        me = lax.axis_index('tp')
        group = lax.axis_index('dp')
        core, chip = me % 2, me // 2
        _, rows, dim = x_in.shape
        heads = w_out.shape[0]
        cols = w_up.shape[1]
        half = cols // 2

        def pick(blocks, index):
            return lax.dynamic_index_in_dim(blocks, index, 0, keepdims=False)

        def to_blocks(value):
            v = [value[s * rows:(s + 1) * rows] for s in range(4)]
            v = [v[0]] + [xor_move(v[s], s) for s in (1, 2, 3)]
            low = [jnp.where(core == 1, a, b) for a, b in ((v[1], v[0]), (v[0], v[1]))]
            high = [jnp.where(core == 1, a, b) for a, b in ((v[3], v[2]), (v[2], v[3]))]
            first = [jnp.where(chip == 1, b, a) for a, b in zip(low, high)]
            last = [jnp.where(chip == 1, a, b) for a, b in zip(low, high)]
            return jnp.stack(first + last)

        x_slots = [pick(x_in, me ^ s) for s in range(4)]
        x_seq = jnp.concatenate([x_slots[0]] + [xor_move(x_slots[s], s) for s in (1, 2, 3)])
        small = jnp.concatenate([b_up, jnp.transpose(b_qkv, (1, 0, 2)).reshape(-1)])
        smalls = [small] + [xor_move(small, s) for s in (1, 2, 3)]
        b_ups = [v[:cols].reshape(2, 1, half) for v in smalls]
        b_qkvs = [v[cols:].reshape(heads, 3, HD) for v in smalls]
        w_heads = jnp.transpose(w_qkv, (0, 2, 3, 1)).reshape(3, heads * HD, dim)
        wq = [w_heads, xor_move(w_heads, 1), xor_move(w_heads, 2)]
        wo = [w_out, xor_move(w_out, 1), xor_move(w_out, 2)]
        dya2 = xor_move(lax.dynamic_slice_in_dim(grad_y, (1 - chip) * 2, 2, 0), 2)
        dy1 = xor_move(grad_y, 1)
        up2 = xor_move(lax.dynamic_slice_in_dim(w_up, group * half, half, 1), 2)
        down2 = xor_move(lax.dynamic_slice_in_dim(w_down, group * half, half, 0), 2)
        ups = [w_up, xor_move(w_up, 1)]
        downs = [w_down, xor_move(w_down, 1)]

        positions = jnp.concatenate([(me ^ s) * rows + jnp.arange(rows) for s in range(4)])
        cos_tab, sin_tab = rope_tables(positions, HD)
        length = jnp.sum((pick(pad_mask, me) > 0).astype(jnp.int32))
        mask_col = jnp.broadcast_to(jnp.where(positions < length, 0.0, NEG_LARGE).astype(F32)[:, None], (4 * rows, LANES))
        x_f = x_seq.astype(F32)
        h1_f, x_hat1, inv_std1 = layer_norm(x_f, ln1_gain, ln1_bias)
        h1 = h1_f.astype(BF16)

        def pair_bias(a, b):
            return jnp.concatenate([a, b], axis=-1)

        fwd_a = attn_fwd(h1, wq[0], wq[1], pair_bias(b_qkvs[0], b_qkvs[1]), cos_tab, sin_tab, mask_col)
        wq.append(xor_move(wq[2], 1))
        fwd_b = attn_fwd(h1, wq[2], wq[3], pair_bias(b_qkvs[2], b_qkvs[3]), cos_tab, sin_tab, mask_col)
        wo.append(xor_move(wo[2], 1))

        def pair_out(a, b):
            return jnp.stack([a, b], axis=1).reshape(2 * heads * HD, dim)

        attn_sum = jnp.dot(fwd_a[3], pair_out(wo[0], wo[1]), preferred_element_type=F32)
        attn_sum = attn_sum + jnp.dot(fwd_b[3], pair_out(wo[2], wo[3]), preferred_element_type=F32)
        x1_f = (x_f + (attn_sum + b_out)).astype(BF16).astype(F32)
        h2_f, x_hat2, inv_std2 = layer_norm(x1_f, ln2_gain, ln2_bias)
        h2 = h2_f.astype(BF16)
        dya3 = xor_move(dya2, 1)
        h2_next = xor_move(h2, 1)
        nxt, oth = me ^ 1, 1 - core
        d_y, d_y_next = join([[(grad_y, me), (dy1, me), (dya2, core), (dya3, core)],
                              [(dy1, nxt), (grad_y, nxt), (dya3, oth), (dya2, oth)]])
        dy_f = d_y.astype(F32)

        def grad_dot(a, b):
            return lax.dot_general(a, b, (((0,), (0,)), ((), ())), preferred_element_type=F32)

        y_a, dh2_a, act0, dpre0, sum0 = mlp_chain(h2, d_y, b_ups[0], ups[:1], downs[:1], emit=True)
        up_y = swap_groups(after(up2, y_a))
        y_a, dh2_a, act1, dpre1, sum1 = mlp_chain(h2, d_y, b_ups[1], ups[1:], downs[1:], before=(y_a, dh2_a), emit=True)
        act_next, dpre_next, sum_next = (xor_move(v, 1) for v in (act1, dpre1, sum1))
        h2_far = xor_move(after(h2, down2), 2)
        dyb2 = xor_move(after(lax.dynamic_slice_in_dim(grad_y, chip * 2, 2, 0), down2), 2)
        own_up, own_down = grad_dot(after(h2, y_a), dpre0), grad_dot(act0, after(d_y, y_a))
        down_y = swap_groups(after(down2, y_a))
        up3, down3 = xor_move(after(up2, y_a), 1), xor_move(after(down2, y_a), 1)
        far_bias = [jnp.where(group == 0, v, v[::-1]) for v in b_ups[2:]]
        y_c, dh2_c = mlp_chain(after(h2, own_up, own_down), d_y, jnp.concatenate([v[:1] for v in far_bias]), [up2, up3], [down2, down3],
                               before=(y_a, dh2_a))
        up3_y, down3_y = xor_move(after(up_y, own_up), 1), xor_move(after(down_y, y_c), 1)
        near_up = own_up + grad_dot(after(h2_next, y_c), dpre_next)
        near_down = own_down + grad_dot(act_next, after(d_y_next, y_c))
        y_d, d_h2 = mlp_chain(after(h2, near_up, near_down), d_y, jnp.concatenate([v[1:] for v in far_bias]), [up_y, up3_y], [down_y, down3_y],
                              before=(y_c, dh2_c))
        y_seq = (x1_f + (y_d + b_down)).astype(BF16)
        y_out = to_blocks(y_seq)
        d_x1 = dy_f + layer_norm_grad(d_h2, x_hat2, inv_std2, ln2_gain)
        d_x1_b = d_x1.astype(BF16)

        def backward(i, fwd, d_mid, first, count):
            q, k, v, o, lse = fwd
            return attn_bwd(h1, d_mid, wq[i], wq[i + 1], wo[i], wo[i + 1], q, k, v, o, lse, cos_tab, sin_tab, mask_col, first, count)

        split = 3
        bwd_b = backward(2, fwd_b, d_x1_b, 0, split)
        g_far = bwd_b[1] + xor_move(bwd_b[2], 1)
        g_across = xor_move(g_far, 2)
        bwd_c = backward(2, fwd_b, after(d_x1_b, g_far), split, heads - split)
        g_far_c = bwd_c[1] + xor_move(bwd_c[2], 1)
        g_across_c = xor_move(g_far_c, 2)
        dyb3 = xor_move(after(dyb2, bwd_b[0]), 1)
        h2_far_next = xor_move(after(h2_far, bwd_b[0]), 1)
        bwd_a = backward(0, fwd_a, after(d_x1_b, g_far_c), 0, heads)
        d_h1 = (bwd_b[0] + bwd_c[0]) + bwd_a[0]
        grad_x_seq = (d_x1 + layer_norm_grad(d_h1, x_hat1, inv_std1, ln1_gain)).astype(BF16)
        sums = jnp.concatenate([jnp.sum(v, axis=0) for v in (dy_f, d_h2 * x_hat2, d_h2, d_x1, d_h1 * x_hat1, d_h1)])
        gb = []
        for part in (bwd_a[3], jnp.concatenate([bwd_b[3], bwd_c[3]])):
            part = jnp.transpose(part[:, :3], (1, 0, 2))
            gb += [part[..., :HD].reshape(-1), part[..., HD:].reshape(-1)]
        packs = [jnp.concatenate([sums, v]) for v in gb]
        packs = [packs[0]] + [xor_move(packs[s], s) for s in (1, 2, 3)]
        totals = (packs[0] + packs[1]) + (packs[2] + packs[3])
        sums, grad_b_qkv = totals[:6 * dim].reshape(6, dim), totals[6 * dim:].reshape(3, heads, HD)
        grad_x = to_blocks(grad_x_seq)

        far, diag = me ^ 2, me ^ 3
        dy_far = join([[(dyb2, core), (dyb3, core), (grad_y, far), (dy1, far), (dyb3, oth), (dyb2, oth), (dy1, diag), (grad_y, diag)]])[0]
        h2_other = jnp.concatenate([after(h2_far, grad_x_seq), h2_far_next])
        pre_act = jnp.dot(h2_other, w_up, preferred_element_type=F32) + b_up
        act, gelu_slope = gelu_terms(pre_act)
        grad_w_down = near_down + grad_dot(act.astype(BF16), dy_far)
        d_pre = lax.dot_general(dy_far, w_down, NT, preferred_element_type=F32) * gelu_slope
        grad_w_up = near_up + grad_dot(h2_other, d_pre.astype(BF16))
        grad_b_up = (sum0[0] + sum_next[0]) + jnp.sum(d_pre, axis=0)
        grads_q, grad_w_out = add_grads(bwd_a[1], xor_move(bwd_a[2], 1), g_across, g_across_c)
        grad_w_qkv = jnp.transpose(grads_q.reshape(3, heads, HD, dim), (0, 3, 1, 2))
        grad_w_out = grad_w_out.reshape(heads, HD, dim)
        return (y_out, grad_x, sums[4], sums[5], grad_w_qkv, grad_b_qkv, grad_w_out, sums[3],
                sums[1], sums[2], grad_w_up, grad_b_up, grad_w_down, sums[0])

    return jax.shard_map(layer, mesh=mesh, in_specs=in_specs, out_specs=out_specs, check_vma=False)
```

```python
import functools

import jax
import jax.numpy as jnp
from jax import lax
from jax.experimental import pallas as pl
from jax.experimental.pallas import tpu as pltpu
from jax.sharding import PartitionSpec as P


LN_EPS = 1e-5
ROPE_BASE = 10000.0
INV_SQRT2 = 0.7071067811865476
INV_SQRT_2PI = 0.3989422804014327
NEG_LARGE = -1e30
F32 = jnp.float32
BF16 = jnp.bfloat16
NT = (((1,), (1,)), ((), ()))
VMEM_LIMIT = 60 << 20
LANES = 128
HD = 64
QB = 256


def layer_norm(values, ln_gain, ln_bias):
    centered = values - jnp.mean(values, axis=-1, keepdims=True)
    inv_std = lax.rsqrt(jnp.mean(centered * centered, axis=-1, keepdims=True) + LN_EPS)
    x_hat = centered * inv_std
    return x_hat * ln_gain + ln_bias, x_hat, inv_std


def layer_norm_grad(d_out, x_hat, inv_std, ln_gain):
    d_hat = d_out * ln_gain
    return inv_std * (d_hat - jnp.mean(d_hat, axis=-1, keepdims=True) - x_hat * jnp.mean(d_hat * x_hat, axis=-1, keepdims=True))


def rope_tables(positions, head_dim):
    half_dim = head_dim // 2
    inv_freq = ROPE_BASE ** (-2.0 * jnp.arange(half_dim, dtype=F32) / head_dim)
    angles = positions.astype(F32)[:, None] * inv_freq[None, :]
    cos_half, sin_half = jnp.cos(angles), jnp.sin(angles)
    cos_tab = jnp.concatenate([cos_half] * 4, axis=-1)
    sin_tab = jnp.concatenate([-sin_half, sin_half, -sin_half, sin_half], axis=-1)
    return cos_tab, sin_tab


def swap_halves(t, first_half):
    return jnp.where(first_half, pltpu.roll(t, 96, 1), pltpu.roll(t, 32, 1))


def pair_rows(ref0, ref1):
    return jnp.concatenate([r[i] for i in range(3) for r in (ref0, ref1)], axis=0)


def attn_fwd_kernel(h_ref, w0_ref, w1_ref, b_ref, cos_ref, sin_ref, mb_ref, q_ref, k_ref, v_ref, o_ref, lse_ref, qs, ks, st):
    seq = h_ref.shape[0]
    lane = lax.broadcasted_iota(jnp.int32, (1, LANES), 1)
    first_half = (lane % HD) < 32
    head0 = lane < HD
    w = pair_rows(w0_ref, w1_ref)
    t = lax.dot_general(h_ref[...], w, NT, preferred_element_type=F32)
    cos, sin = cos_ref[...], sin_ref[...]
    tq = (t[:, :LANES] + b_ref[0, 0:1]) * 0.125
    tk = t[:, LANES:256] + b_ref[0, 1:2]
    q = (tq * cos + swap_halves(tq, first_half) * sin).astype(BF16)
    k = (tk * cos + swap_halves(tk, first_half) * sin).astype(BF16)
    v_ref[...] = (t[:, 256:] + b_ref[0, 2:3]).astype(BF16)
    q_ref[...] = q
    k_ref[...] = k
    q, k = q.astype(F32), k.astype(F32)
    mb = mb_ref[...]
    qs[0] = jnp.where(head0, q, jnp.where(lane == HD, 1.0, 0.0)).astype(BF16)
    qs[1] = jnp.where(head0, jnp.where(lane == 0, 1.0, 0.0), q).astype(BF16)
    ks[0] = jnp.where(head0, k, jnp.where(lane == HD, mb, 0.0)).astype(BF16)
    ks[1] = jnp.where(head0, jnp.where(lane == 0, mb, 0.0), k).astype(BF16)

    def block(j, carry):
        rows = pl.ds(pl.multiple_of(j * QB, QB), QB)
        outs, stats = [], []
        for head in range(2):
            s = lax.dot_general(qs[head, rows, :], ks[head], NT, preferred_element_type=F32)
            m = jnp.max(s, axis=-1, keepdims=True)
            e = jnp.exp(s - m)
            total = jnp.sum(e, axis=-1, keepdims=True)
            p = (e * (1.0 / total)).astype(BF16)
            outs.append(jnp.dot(p, v_ref[...], preferred_element_type=F32))
            stats.append(m + jnp.log(total))
        o_ref[rows, :] = jnp.where(head0, outs[0], outs[1]).astype(BF16)
        st[rows, :] = jnp.where(head0, stats[0], stats[1])
        return carry

    lax.fori_loop(0, seq // QB, block, 0)
    st_t = st[...].T
    lse_ref[0] = jnp.concatenate([st_t[0:1]] * 4 + [st_t[HD:65]] * 4, axis=0)


def whole(*shape):
    return pl.BlockSpec(shape, lambda *i: (0,) * len(shape))


def head_blocks(parts, dim, first=0):
    return pl.BlockSpec((parts, HD, dim), lambda i: (0, i + first, 0))


def compiler_params():
    return pltpu.CompilerParams(dimension_semantics=("arbitrary",), vmem_limit_bytes=VMEM_LIMIT)


def cost(flops):
    return pl.CostEstimate(flops=flops, bytes_accessed=20_000_000, transcendentals=0)


def attn_fwd(h1, w0, w1, bias, cos_tab, sin_tab, mask_col):
    seq, dim = h1.shape
    heads = w0.shape[1] // HD
    pair = pl.BlockSpec((seq, LANES), lambda i: (0, i))
    head_w = head_blocks(3, dim)
    tab = whole(seq, LANES)
    act = jax.ShapeDtypeStruct((seq, heads * LANES), BF16)
    both = pltpu.VMEM((2, seq, LANES), BF16)
    return pl.pallas_call(
        attn_fwd_kernel,
        grid=(heads,),
        in_specs=[whole(seq, dim), head_w, head_w, pl.BlockSpec((1, 3, LANES), lambda i: (i, 0, 0)), tab, tab, tab],
        out_specs=[pair, pair, pair, pair, pl.BlockSpec((1, 8, seq), lambda i: (i, 0, 0))],
        out_shape=[act, act, act, act, jax.ShapeDtypeStruct((heads, 8, seq), F32)],
        scratch_shapes=[both, both, pltpu.VMEM((seq, LANES), F32)],
        compiler_params=compiler_params(),
        cost_estimate=cost(heads * seq * (dim + seq) * 1024),
        name="attn_fwd",
    )(h1, w0, w1, bias, cos_tab, sin_tab, mask_col)


def attn_bwd_kernel(h_ref, dx_ref, w0_ref, w1_ref, wo0_ref, wo1_ref, q_ref, k_ref, v_ref, o_ref, lse_ref, cos_ref, sin_ref, mb_ref,
                    dh_ref, gw0_ref, gw1_ref, gb_ref, qs, qz, ks, dos, kt, dqt, dk_acc, dv_acc):
    seq, _ = h_ref.shape
    lane = lax.broadcasted_iota(jnp.int32, (1, LANES), 1)
    first_half = (lane % HD) < 32
    head0 = lane < HD
    dx = dx_ref[...]
    wo = jnp.concatenate([wo0_ref[0], wo1_ref[0]], axis=0)
    d_o = lax.dot_general(dx, wo, NT, preferred_element_type=F32)
    dos[0] = jnp.where(head0, d_o, 0.0).astype(BF16)
    dos[1] = jnp.where(head0, 0.0, d_o).astype(BF16)
    gwo = jnp.dot(o_ref[...].T, dx, preferred_element_type=F32)
    gw0_ref[3] = gwo[:HD]
    gw1_ref[3] = gwo[HD:]
    q, k, mb = q_ref[...].astype(F32), k_ref[...].astype(F32), mb_ref[...]
    qs[0] = jnp.where(head0, q, jnp.where(lane == HD, 1.0, 0.0)).astype(BF16)
    qs[1] = jnp.where(head0, jnp.where(lane == 0, 1.0, 0.0), q).astype(BF16)
    qz[0] = jnp.where(head0, q, 0.0).astype(BF16)
    qz[1] = jnp.where(head0, 0.0, q).astype(BF16)
    ks[0] = jnp.where(head0, k, jnp.where(lane == HD, mb, 0.0)).astype(BF16)
    ks[1] = jnp.where(head0, jnp.where(lane == 0, mb, 0.0), k).astype(BF16)
    kt[...] = k_ref[...].T
    dk_acc[...] = jnp.zeros_like(dk_acc)
    dv_acc[...] = jnp.zeros_like(dv_acc)

    def block(j, carry):
        rows = pl.ds(pl.multiple_of(j * QB, QB), QB)
        for head in range(2):
            s_t = lax.dot_general(ks[head], qs[head, rows, :], NT, preferred_element_type=F32)
            p_t = jnp.exp(s_t - lse_ref[0, 4 * head:4 * head + 1, rows])
            do_b = dos[head, rows, :]
            dp_t = lax.dot_general(v_ref[...], do_b, NT, preferred_element_type=F32)
            corr = jnp.sum(p_t * dp_t, axis=0, keepdims=True)
            ds_t = (p_t * (dp_t - corr)).astype(BF16)
            dv_acc[...] += jnp.dot(p_t.astype(BF16), do_b, preferred_element_type=F32)
            dk_acc[...] += jnp.dot(ds_t, qz[head, rows, :], preferred_element_type=F32)
            dqt[HD * head:HD * head + HD, rows] = jnp.dot(kt[HD * head:HD * head + HD, :], ds_t, preferred_element_type=F32)
        return carry

    lax.fori_loop(0, seq // QB, block, 0)
    cos, sin = cos_ref[...], sin_ref[...]
    dq, dk, dv = dqt[...].T, dk_acc[...], dv_acc[...]
    dq = (dq * cos - swap_halves(dq, first_half) * sin) * 0.125
    dk = dk * cos - swap_halves(dk, first_half) * sin
    d_all = jnp.concatenate([dq, dk, dv], axis=1)
    sums = jnp.sum(d_all, axis=0, keepdims=True)
    gb_ref[0] = jnp.concatenate([sums[:, :LANES], sums[:, LANES:256], sums[:, 256:], jnp.zeros((5, LANES), F32)], axis=0)
    d_low = d_all.astype(BF16)
    w = pair_rows(w0_ref, w1_ref)
    gw = jnp.dot(d_low.T, h_ref[...], preferred_element_type=F32)
    for i in range(3):
        gw0_ref[i] = gw[LANES * i:LANES * i + HD]
        gw1_ref[i] = gw[LANES * i + HD:LANES * (i + 1)]

    @pl.when(pl.program_id(0) == 0)
    def _():
        dh_ref[...] = jnp.zeros_like(dh_ref)

    dh_ref[...] += jnp.dot(d_low, w, preferred_element_type=F32)


def attn_bwd(h1, d_x1, w0, w1, wo0, wo1, q, k, v, o, lse, cos_tab, sin_tab, mask_col, first, count):
    seq, dim = h1.shape
    pair = pl.BlockSpec((seq, LANES), lambda i: (0, i + first))
    head_w = head_blocks(3, dim, first)
    head_o = pl.BlockSpec((1, HD, dim), lambda i: (i + first, 0, 0))
    tab = whole(seq, LANES)
    gw = jax.ShapeDtypeStruct((4, count * HD, dim), F32)
    half = pltpu.VMEM((2, seq, LANES), BF16)
    acc = pltpu.VMEM((seq, LANES), F32)
    return pl.pallas_call(
        attn_bwd_kernel,
        grid=(count,),
        in_specs=[whole(seq, dim), whole(seq, dim), head_w, head_w, head_o, head_o, pair, pair, pair, pair,
                  pl.BlockSpec((1, 8, seq), lambda i: (i + first, 0, 0)), tab, tab, tab],
        out_specs=[whole(seq, dim), head_blocks(4, dim), head_blocks(4, dim), pl.BlockSpec((1, 8, LANES), lambda i: (i, 0, 0))],
        out_shape=[jax.ShapeDtypeStruct((seq, dim), F32), gw, gw, jax.ShapeDtypeStruct((count, 8, LANES), F32)],
        scratch_shapes=[half, half, half, half, pltpu.VMEM((LANES, seq), BF16), pltpu.VMEM((LANES, seq), F32), acc, acc],
        compiler_params=compiler_params(),
        cost_estimate=cost(count * seq * (dim + seq) * 2048),
        name="attn_bwd",
    )(h1, d_x1, w0, w1, wo0, wo1, q, k, v, o, lse, cos_tab, sin_tab, mask_col)


def gelu_terms(pre):
    erf_term = lax.erf(pre * INV_SQRT2)
    act = 0.5 * pre * (1.0 + erf_term)
    slope = 0.5 * (1.0 + erf_term) + pre * jnp.exp(-0.5 * pre * pre) * INV_SQRT_2PI
    return act, slope


def mlp_kernel(n_w, chained, emit, chain, *refs):
    refs = list(refs)
    take = lambda n: [refs.pop(0) for _ in range(n)]
    h_ref, dy_ref, b_ref = take(3)
    ups, downs = take(n_w), take(n_w)
    before = take(2) if chained else None
    y_ref, dh_ref = take(2) if chain else (None, None)
    act_ref, dpre_ref, sum_ref = take(3) if emit else (None,) * 3
    wu, wd, sem = refs
    step = pl.program_id(0)
    width = wu.shape[0] // n_w
    copies = []
    for t in range(n_w):
        cols = pl.ds(t * width, width)
        copies.append((pltpu.make_async_copy(ups[t], wu.at[:, cols], sem.at[0, t]), pltpu.make_async_copy(downs[t], wd.at[cols, :], sem.at[1, t])))

    @pl.when(step == 0)
    def _():
        for up, down in copies:
            up.start()
            down.start()

    @pl.when(step == 0)
    def _():
        for up, down in copies:
            up.wait()
            down.wait()

    pre = jnp.dot(h_ref[...], wu[...], preferred_element_type=F32) + b_ref[...]
    act, slope = gelu_terms(pre)
    act = act.astype(BF16)
    d_pre = lax.dot_general(dy_ref[...], wd[...], NT, preferred_element_type=F32) * slope
    d_low = d_pre.astype(BF16)
    if chain:
        y_part = jnp.dot(act, wd[...], preferred_element_type=F32)
        dh_part = lax.dot_general(d_low, wu[...], NT, preferred_element_type=F32)
        y_ref[...] = before[0][...] + y_part if chained else y_part
        dh_ref[...] = before[1][...] + dh_part if chained else dh_part
    if emit:
        act_ref[...] = act
        dpre_ref[...] = d_low
        total = jnp.broadcast_to(jnp.sum(d_pre, axis=0, keepdims=True), sum_ref.shape)
        sum_ref[...] = total + jnp.where(step == 0, 0.0, sum_ref[...])


def mlp_chain(h2, d_y, bias, ups, downs, before=(), emit=False, chain=True):
    seq, dim = h2.shape
    bias = bias.reshape(1, -1)
    width = bias.shape[1]
    rows = pl.BlockSpec((QB, dim), lambda j: (j, 0))
    wide = pl.BlockSpec((QB, width), lambda j: (j, 0))
    hbm = pl.BlockSpec(memory_space=pl.ANY)
    out = jax.ShapeDtypeStruct((seq, dim), F32)
    low = jax.ShapeDtypeStruct((seq, width), BF16)
    out_specs, out_shape = ([rows, rows], [out, out]) if chain else ([], [])
    if emit:
        out_specs += [wide, wide, whole(8, width)]
        out_shape += [low, low, jax.ShapeDtypeStruct((8, width), F32)]
    return pl.pallas_call(
        functools.partial(mlp_kernel, len(ups), bool(before), emit, chain),
        grid=(seq // QB,),
        in_specs=[rows, rows, whole(1, width)] + [hbm] * (2 * len(ups)) + [rows] * len(before),
        out_specs=out_specs,
        out_shape=out_shape,
        scratch_shapes=[pltpu.VMEM((dim, width), BF16), pltpu.VMEM((width, dim), BF16), pltpu.SemaphoreType.DMA((2, len(ups)))],
        compiler_params=compiler_params(),
        cost_estimate=cost(8 * seq * dim * width),
        name="mlp_chain",
    )(h2, d_y, bias, *ups, *downs, *before)


def join_kernel(places, n_src, idx_ref, *refs):
    srcs, outs, sem = refs[:n_src], refs[n_src:-1], refs[-1]
    rows = srcs[0].shape[1]
    copies = []
    for p, (src, out, slot) in enumerate(places):
        copies.append(pltpu.make_async_copy(srcs[src].at[idx_ref[p]], outs[out].at[pl.ds(slot * rows, rows)], sem.at[p]))
    for c in copies:
        c.start()
    for c in copies:
        c.wait()


def join(pieces):
    arrays, places, index = [], [], []
    for out, row in enumerate(pieces):
        for slot, (array, i) in enumerate(row):
            at = [k for k, a in enumerate(arrays) if a is array]
            if not at:
                arrays.append(array)
            places.append((at[0] if at else len(arrays) - 1, out, slot))
            index.append(i)
    _, rows, dim = arrays[0].shape
    out = jax.ShapeDtypeStruct((len(pieces[0]) * rows, dim), arrays[0].dtype)
    vmem = pl.BlockSpec(memory_space=pltpu.VMEM)
    return pl.pallas_call(
        functools.partial(join_kernel, places, len(arrays)),
        in_specs=[pl.BlockSpec(memory_space=pltpu.SMEM)] + [pl.BlockSpec(memory_space=pl.ANY)] * len(arrays),
        out_specs=[vmem] * len(pieces),
        out_shape=[out] * len(pieces),
        scratch_shapes=[pltpu.SemaphoreType.DMA((len(places),))],
        cost_estimate=cost(10_000_000),
        name="join_rows",
    )(jnp.stack(index).astype(jnp.int32), *arrays)


def add_kernel(split, a_ref, b_ref, c0_ref, c1_ref, q_ref, o_ref):
    part = pl.program_id(0)

    def store(dst):
        dst[:split] = (a_ref[0, :split] + b_ref[0, :split]) + c0_ref[0]
        dst[split:] = (a_ref[0, split:] + b_ref[0, split:]) + c1_ref[0]

    @pl.when(part < 3)
    def _():
        store(q_ref.at[0])

    @pl.when(part == 3)
    def _():
        store(o_ref)


def add_grads(a, b, c0, c1):
    parts, size, dim = a.shape
    last = parts - 1
    block = lambda v: pl.BlockSpec((1,) + v.shape[1:], lambda p: (p, 0, 0))
    return pl.pallas_call(
        functools.partial(add_kernel, c0.shape[1]),
        grid=(parts,),
        in_specs=[block(a), block(b), block(c0), block(c1)],
        out_specs=[pl.BlockSpec((1, size, dim), lambda p: (jnp.minimum(p, last - 1), 0, 0)), whole(size, dim)],
        out_shape=[jax.ShapeDtypeStruct((last, size, dim), F32), jax.ShapeDtypeStruct((size, dim), F32)],
        compiler_params=compiler_params(),
        cost_estimate=cost(10_000_000),
        name="add_grads",
    )(a, b, c0, c1)


def xor_move(value, bits):
    return lax.ppermute(value, 'tp', [(i, i ^ bits) for i in range(4)])


def swap_groups(value):
    return lax.ppermute(value, 'dp', [(0, 1), (1, 0)])


def after(value, *others):
    return lax.optimization_barrier((value,) + others)[0]


def solution(mesh):
    act_spec = P('dp', 'tp', None)
    rep_vec = P(None)
    part_vec = P('dp')
    in_specs = (act_spec, act_spec, P('dp', None), rep_vec, rep_vec, P(None, None, 'tp', None), P(None, 'tp', None),
                P('tp', None, None), rep_vec, rep_vec, rep_vec, P(None, 'tp'), P('tp'), P('tp', None), rep_vec)
    out_specs = (act_spec, act_spec, part_vec, part_vec, P('dp', None, 'tp', None), P('dp', 'tp', None),
                 P(('dp', 'tp'), None, None), part_vec, part_vec, part_vec, P('dp', 'tp'), P(('dp', 'tp')),
                 P(('dp', 'tp'), None), part_vec)

    def layer(x_in, grad_y, pad_mask, ln1_gain, ln1_bias, w_qkv, b_qkv, w_out, b_out, ln2_gain, ln2_bias, w_up, b_up, w_down, b_down):
        me = lax.axis_index('tp')
        group = lax.axis_index('dp')
        core, chip = me % 2, me // 2
        _, rows, dim = x_in.shape
        heads = w_out.shape[0]
        cols = w_up.shape[1]
        half = cols // 2

        def pick(blocks, index):
            return lax.dynamic_index_in_dim(blocks, index, 0, keepdims=False)

        def to_blocks(value):
            v = [value[s * rows:(s + 1) * rows] for s in range(4)]
            v = [v[0]] + [xor_move(v[s], s) for s in (1, 2, 3)]
            low = [jnp.where(core == 1, a, b) for a, b in ((v[1], v[0]), (v[0], v[1]))]
            high = [jnp.where(core == 1, a, b) for a, b in ((v[3], v[2]), (v[2], v[3]))]
            first = [jnp.where(chip == 1, b, a) for a, b in zip(low, high)]
            last = [jnp.where(chip == 1, a, b) for a, b in zip(low, high)]
            return jnp.stack(first + last)

        x_slots = [pick(x_in, me ^ s) for s in range(4)]
        x_seq = jnp.concatenate([x_slots[0]] + [xor_move(x_slots[s], s) for s in (1, 2, 3)])
        small = jnp.concatenate([b_up, jnp.transpose(b_qkv, (1, 0, 2)).reshape(-1)])
        smalls = [small] + [xor_move(small, s) for s in (1, 2, 3)]
        b_ups = [v[:cols].reshape(2, 1, half) for v in smalls]
        b_qkvs = [v[cols:].reshape(heads, 3, HD) for v in smalls]
        w_heads = jnp.transpose(w_qkv, (0, 2, 3, 1)).reshape(3, heads * HD, dim)
        wq = [w_heads, xor_move(w_heads, 1), xor_move(w_heads, 2)]
        wo = [w_out, xor_move(w_out, 1), xor_move(w_out, 2)]
        dya2 = xor_move(lax.dynamic_slice_in_dim(grad_y, (1 - chip) * 2, 2, 0), 2)
        dy1 = xor_move(grad_y, 1)
        up2 = xor_move(lax.dynamic_slice_in_dim(w_up, group * half, half, 1), 2)
        down2 = xor_move(lax.dynamic_slice_in_dim(w_down, group * half, half, 0), 2)
        ups = [w_up, xor_move(w_up, 1)]
        downs = [w_down, xor_move(w_down, 1)]

        positions = jnp.concatenate([(me ^ s) * rows + jnp.arange(rows) for s in range(4)])
        cos_tab, sin_tab = rope_tables(positions, HD)
        length = jnp.sum((pick(pad_mask, me) > 0).astype(jnp.int32))
        mask_col = jnp.broadcast_to(jnp.where(positions < length, 0.0, NEG_LARGE).astype(F32)[:, None], (4 * rows, LANES))
        x_f = x_seq.astype(F32)
        h1_f, x_hat1, inv_std1 = layer_norm(x_f, ln1_gain, ln1_bias)
        h1 = h1_f.astype(BF16)

        def pair_bias(a, b):
            return jnp.concatenate([a, b], axis=-1)

        fwd_a = attn_fwd(h1, wq[0], wq[1], pair_bias(b_qkvs[0], b_qkvs[1]), cos_tab, sin_tab, mask_col)
        wq.append(xor_move(wq[2], 1))
        fwd_b = attn_fwd(h1, wq[2], wq[3], pair_bias(b_qkvs[2], b_qkvs[3]), cos_tab, sin_tab, mask_col)
        wo.append(xor_move(wo[2], 1))

        def pair_out(a, b):
            return jnp.stack([a, b], axis=1).reshape(2 * heads * HD, dim)

        attn_sum = jnp.dot(fwd_a[3], pair_out(wo[0], wo[1]), preferred_element_type=F32)
        attn_sum = attn_sum + jnp.dot(fwd_b[3], pair_out(wo[2], wo[3]), preferred_element_type=F32)
        x1_f = (x_f + (attn_sum + b_out)).astype(BF16).astype(F32)
        h2_f, x_hat2, inv_std2 = layer_norm(x1_f, ln2_gain, ln2_bias)
        h2 = h2_f.astype(BF16)
        dya3 = xor_move(dya2, 1)
        h2_next = xor_move(h2, 1)
        nxt, oth = me ^ 1, 1 - core
        d_y, d_y_next = join([[(grad_y, me), (dy1, me), (dya2, core), (dya3, core)],
                              [(dy1, nxt), (grad_y, nxt), (dya3, oth), (dya2, oth)]])
        dy_f = d_y.astype(F32)

        def grad_dot(a, b):
            return lax.dot_general(a, b, (((0,), (0,)), ((), ())), preferred_element_type=F32)

        y_a, dh2_a, act0, dpre0, sum0 = mlp_chain(h2, d_y, b_ups[0], ups[:1], downs[:1], emit=True)
        up_y = swap_groups(after(up2, y_a))
        y_a, dh2_a, act1, dpre1, sum1 = mlp_chain(h2, d_y, b_ups[1], ups[1:], downs[1:], before=(y_a, dh2_a), emit=True)
        act_next, dpre_next, sum_next = (xor_move(v, 1) for v in (act1, dpre1, sum1))
        h2_far = xor_move(after(h2, down2), 2)
        dyb2 = xor_move(after(lax.dynamic_slice_in_dim(grad_y, chip * 2, 2, 0), down2), 2)
        own_up, own_down = grad_dot(after(h2, y_a), dpre0), grad_dot(act0, after(d_y, y_a))
        down_y = swap_groups(after(down2, y_a))
        up3, down3 = xor_move(after(up2, y_a), 1), xor_move(after(down2, y_a), 1)
        far_bias = [jnp.where(group == 0, v, v[::-1]) for v in b_ups[2:]]
        y_c, dh2_c = mlp_chain(after(h2, own_up, own_down), d_y, jnp.concatenate([v[:1] for v in far_bias]), [up2, up3], [down2, down3],
                               before=(y_a, dh2_a))
        up3_y, down3_y = xor_move(after(up_y, own_up), 1), xor_move(after(down_y, y_c), 1)
        near_up = own_up + grad_dot(after(h2_next, y_c), dpre_next)
        near_down = own_down + grad_dot(act_next, after(d_y_next, y_c))
        y_d, d_h2 = mlp_chain(after(h2, near_up, near_down), d_y, jnp.concatenate([v[1:] for v in far_bias]), [up_y, up3_y], [down_y, down3_y],
                              before=(y_c, dh2_c))
        y_seq = (x1_f + (y_d + b_down)).astype(BF16)
        y_out = to_blocks(y_seq)
        d_x1 = dy_f + layer_norm_grad(d_h2, x_hat2, inv_std2, ln2_gain)
        d_x1_b = d_x1.astype(BF16)

        def backward(i, fwd, d_mid, first, count):
            q, k, v, o, lse = fwd
            return attn_bwd(h1, d_mid, wq[i], wq[i + 1], wo[i], wo[i + 1], q, k, v, o, lse, cos_tab, sin_tab, mask_col, first, count)

        split = 3
        bwd_b = backward(2, fwd_b, d_x1_b, 0, split)
        g_far = bwd_b[1] + xor_move(bwd_b[2], 1)
        g_across = xor_move(g_far, 2)
        bwd_c = backward(2, fwd_b, after(d_x1_b, g_far), split, heads - split)
        g_far_c = bwd_c[1] + xor_move(bwd_c[2], 1)
        g_across_c = xor_move(g_far_c, 2)
        dyb3 = xor_move(after(dyb2, bwd_b[0]), 1)
        h2_far_next = xor_move(after(h2_far, bwd_b[0]), 1)
        bwd_a = backward(0, fwd_a, after(d_x1_b, g_far_c), 0, heads)
        d_h1 = (bwd_b[0] + bwd_c[0]) + bwd_a[0]
        grad_x_seq = (d_x1 + layer_norm_grad(d_h1, x_hat1, inv_std1, ln1_gain)).astype(BF16)
        sums = jnp.stack([jnp.sum(v, axis=0) for v in (dy_f, d_h2 * x_hat2, d_h2, d_x1, d_h1 * x_hat1, d_h1)])
        gb = []
        for part in (bwd_a[3], jnp.concatenate([bwd_b[3], bwd_c[3]])):
            part = jnp.transpose(part[:, :3], (1, 0, 2))
            gb += [part[..., :HD], part[..., HD:]]
        sums = [sums] + [xor_move(sums, s) for s in (1, 2, 3)]
        sums = (sums[0] + sums[1]) + (sums[2] + sums[3])
        gb = [gb[0]] + [xor_move(gb[s], s) for s in (1, 2, 3)]
        grad_b_qkv = (gb[0] + gb[1]) + (gb[2] + gb[3])
        grad_x = to_blocks(grad_x_seq)

        far, diag = me ^ 2, me ^ 3
        dy_far = join([[(dyb2, core), (dyb3, core), (grad_y, far), (dy1, far), (dyb3, oth), (dyb2, oth), (dy1, diag), (grad_y, diag)]])[0]
        h2_other = jnp.concatenate([after(h2_far, grad_x_seq), h2_far_next])
        act, d_pre, sum_far = mlp_chain(h2_other, dy_far, b_ups[0], ups[:1], downs[:1], emit=True, chain=False)
        grad_w_down = near_down + grad_dot(act, dy_far)
        grad_w_up = near_up + grad_dot(h2_other, d_pre)
        grad_b_up = (sum0[0] + sum_next[0]) + sum_far[0]
        grads_q, grad_w_out = add_grads(bwd_a[1], xor_move(bwd_a[2], 1), g_across, g_across_c)
        grad_w_qkv = jnp.transpose(grads_q.reshape(3, heads, HD, dim), (0, 3, 1, 2))
        grad_w_out = grad_w_out.reshape(heads, HD, dim)
        return (y_out, grad_x, sums[4], sums[5], grad_w_qkv, grad_b_qkv, grad_w_out, sums[3],
                sums[1], sums[2], grad_w_up, grad_b_up, grad_w_down, sums[0])

    return jax.shard_map(layer, mesh=mesh, in_specs=in_specs, out_specs=out_specs, check_vma=False)
```
